32 devices in a mesh: group: 8 (over z, core), helper: 4 (over y, x).
Axes of the slice: x: 2, y: 2, z: 4, core: 2. Of those that a mesh axis runs over, the one named last changes fastest.
Arguments:
- candidates: bfloat16 [64, 128, 1024], P(('group', 'helper')), may hold values from -36 to 36
- block_user: int32 [64], P(('group', 'helper')), may hold values from 0 to 3, as said below
- live_rows: int32 [64], P(('group', 'helper')), may hold values from 1 to 128
- prefix_keys: bfloat16 [32, 256, 1024], P(('group', 'helper')), may hold values from -6 to 6
- prefix_values: bfloat16 [32, 256, 1024], P(('group', 'helper')), may hold values from -6 to 6
- w_proj: bfloat16 [1024, 4096], P(('group', 'helper')), may hold values from -0.1875 to 0.1875
- w_out: bfloat16 [1024, 1024], P(('group', 'helper')), may hold values from -0.1875 to 0.1875
- gain_in: float32 [1024], replicated, may hold values from 0.1 to 1.9
- gain_mid: float32 [1024], replicated, may hold values from 0.1 to 1.9
- score_vec: float32 [1024], replicated, may hold values from -0.1875 to 0.1875
Outputs:
- embeddings: bfloat16 [64, 128, 1024], P(('group', 'helper'))
- scores: float32 [64, 128], P(('group', 'helper'))
The draws below stay inside these ranges and needn't reach their ends.
Inputs may be any that keep to these rules, and one draw needn't show every extreme that they name: `block_user`: the 2 blocks of one device name different users; in every group some user is named by a block of every device of the group.
All inputs are finite; a program needn't handle non-finite values.
Results may differ from the reference program's by a relative error of at most 0.0045.
Values may be sent and summed in bfloat16 or wider, within the bound.
No kernel may reach another device: no remote copies, remote signals or barrier semaphores. Data moves between devices by JAX's collectives and lax.ppermute only.
A program may use at most 128 MiB of HBM per device.

```python
import math
import jax
import jax.numpy as jnp
from jax import lax

D = 1024
HEADS = 8
ROWS = 128
PREFIX = 256
BLK_DEV = 2
BLOCKS = 64
USERS = 32
N_GROUP = 8
N_HELPER = 4


def assignment(key):
    base_key = jax.random.fold_in(key, 7)
    key_hot, key_rank, key_place, key_live = jax.random.split(base_key, 4)
    device_count = N_GROUP * N_HELPER
    hot_user = jax.random.randint(key_hot, (N_GROUP, 1), 0, N_HELPER).astype(jnp.int32)
    hot_device = jnp.repeat(hot_user, N_HELPER, axis=0)
    rank_keys = jax.random.split(key_rank, device_count)
    rank_table = jax.vmap(lambda piece_key: jax.random.permutation(piece_key, N_HELPER))(rank_keys).astype(jnp.int32)
    user_ids = jnp.arange(N_HELPER, dtype=jnp.int32)[None, :]
    rank_table = jnp.where(user_ids == hot_device, -1, rank_table)
    ordering = jnp.argsort(rank_table, axis=1, stable=True).astype(jnp.int32)
    chosen = ordering[:, :BLK_DEV]
    place_keys = jax.random.split(key_place, device_count)
    positions = jax.vmap(lambda piece_key: jax.random.permutation(piece_key, BLK_DEV))(place_keys).astype(jnp.int32)
    chosen = jnp.take_along_axis(chosen, positions, axis=1)
    lives = jax.random.randint(key_live, (device_count, BLK_DEV), 1, ROWS + 1).astype(jnp.int32)
    lives = jnp.where(chosen == hot_device, ROWS, lives)
    return (chosen.reshape(-1).astype(jnp.int32), lives.reshape(-1).astype(jnp.int32))


def draw_block_user(key, part):
    return assignment(key)[0]


def draw_live_rows(key, part):
    return assignment(key)[1]


def draw_candidates(key, part):
    base_key = jax.random.fold_in(key, 11)
    key_base, key_row, key_col = jax.random.split(base_key, 3)
    dims_full = (BLOCKS, ROWS, D)
    row_scale = jnp.exp(jax.random.uniform(key_row, (BLOCKS, ROWS, 1), jnp.float32, math.log(0.3), math.log(3.0)))
    col_scale = jnp.exp(jax.random.uniform(key_col, (1, 1, D), jnp.float32, math.log(0.3), math.log(3.0)))
    base_draw = jnp.clip(jax.random.normal(key_base, dims_full, jnp.float32), -4.0, 4.0)
    return (base_draw * row_scale * col_scale).astype(jnp.bfloat16)


def steps_of(own_key, extent, shards, smallest, top_value):
    level, own = 1.0, jax.random.fold_in(own_key, 6)
    for axis_at, parts in shards:
        draws = jnp.exp(jax.random.uniform(jax.random.fold_in(own, axis_at), (parts,), jnp.float32, smallest / len(shards), top_value / len(shards)))
        level = level * jnp.repeat(draws, extent[axis_at] // parts).reshape([-1 if axis == axis_at else 1 for axis in range(len(extent))])
    return level


def scatter_about(rng, shape, scale, most, cuts=(), kind=jnp.bfloat16):
    drawn = scale * jax.random.normal(rng, shape, jnp.float32)
    if cuts:
        drawn = drawn * steps_of(rng, shape, cuts, -0.22, 0.18)
    return jnp.clip(drawn, -most, most).astype(kind)


def setup_inputs(seed: int = 0) -> dict:
    streams_of = jax.random.split(jax.random.key(seed), 11)
    candidates = draw_candidates(jax.random.fold_in(streams_of[10], 71), 0)
    block_user = draw_block_user(jax.random.fold_in(streams_of[10], 71), 0)
    live_rows = draw_live_rows(jax.random.fold_in(streams_of[10], 71), 0)
    prefix_keys = scatter_about(streams_of[3], (USERS, PREFIX, D), 1.0, 6.0, ((0, 32),))
    prefix_values = scatter_about(streams_of[4], (USERS, PREFIX, D), 1.0, 6.0, ((0, 32),))
    w_proj = scatter_about(streams_of[5], (D, 4 * D), D ** -0.5, 0.1875, ((0, 32),))
    w_out = scatter_about(streams_of[6], (D, D), D ** -0.5, 0.1875, ((0, 32),))
    gain_in = jnp.clip(1.0 + 0.18 * jax.random.normal(streams_of[7], (D,), jnp.float32), 0.1, 1.9)
    gain_mid = jnp.clip(1.0 + 0.18 * jax.random.normal(streams_of[8], (D,), jnp.float32), 0.1, 1.9)
    score_vec = scatter_about(streams_of[9], (D,), D ** -0.5, 0.1875, (), jnp.float32)
    return dict(candidates=candidates, block_user=block_user, live_rows=live_rows, prefix_keys=prefix_keys, prefix_values=prefix_values, w_proj=w_proj, w_out=w_out, gain_in=gain_in, gain_mid=gain_mid, score_vec=score_vec)


epsilon = 1e-05

def layer_norm(values, gain):
    average = lax.optimization_barrier(jnp.mean(values, axis=-1, keepdims=True))
    centred = values - average
    spread = lax.optimization_barrier(jnp.mean(centred * centred, axis=-1, keepdims=True))
    return centred * lax.rsqrt(spread + epsilon) * gain

def reference(candidates, block_user, live_rows, prefix_keys, prefix_values, w_proj, w_out, gain_in, gain_mid, score_vec):
    head_dim = D // HEADS
    score_scale = head_dim ** (-0.5)
    device_count = N_GROUP * N_HELPER
    owners_all = jnp.arange(BLOCKS, dtype=jnp.int32) // (BLK_DEV * N_HELPER) * N_HELPER + block_user.astype(jnp.int32)
    grouped = (candidates.reshape(device_count, BLK_DEV, ROWS, D), owners_all.reshape(device_count, BLK_DEV), live_rows.reshape(device_count, BLK_DEV))

    def one_device(inputs):
        cand_blocks, owners, lives = inputs
        cand_rows = cand_blocks.reshape(BLK_DEV * ROWS, D).astype(jnp.float32)
        normed = layer_norm(cand_rows, gain_in).astype(jnp.bfloat16)
        projected = jax.nn.silu(jnp.dot(normed, w_proj, preferred_element_type=jnp.float32))
        gate_portion = projected[:, :D]
        value_part = projected[:, D:2 * D]
        query_portion = projected[:, 2 * D:3 * D]
        key_part = projected[:, 3 * D:]
        query_bf = lax.optimization_barrier(query_portion.astype(jnp.bfloat16))
        query_heads = query_bf.astype(jnp.float32).reshape(-1, HEADS, head_dim)
        own_weight = jax.nn.silu(score_scale * lax.optimization_barrier(jnp.sum(query_heads * key_part.reshape(-1, HEADS, head_dim), axis=-1)))
        own_term = (own_weight[..., None] * value_part.reshape(-1, HEADS, head_dim)).reshape(-1, D)
        key_sel = jnp.take(prefix_keys, owners, axis=0).astype(jnp.float32).reshape(BLK_DEV, PREFIX, HEADS, head_dim)
        selected_values = jnp.take(prefix_values, owners, axis=0).astype(jnp.float32).reshape(BLK_DEV, PREFIX, HEADS, head_dim)
        query_blocks = query_heads.reshape(BLK_DEV, ROWS, HEADS, head_dim)
        raw_scores = jnp.einsum('brhd,bphd->bhrp', query_blocks, key_sel)
        weight_brainfloat = lax.optimization_barrier(jax.nn.silu(score_scale * raw_scores).astype(jnp.bfloat16))
        prefix_mix = jnp.einsum('bhrp,bphd->brhd', weight_brainfloat.astype(jnp.float32), selected_values)
        prefix_bf = lax.optimization_barrier(prefix_mix.astype(jnp.bfloat16))
        mixed = prefix_bf.astype(jnp.float32).reshape(-1, D) + own_term
        gated = (layer_norm(mixed, gain_mid) * gate_portion).astype(jnp.bfloat16)
        updated = cand_rows + jnp.dot(gated, w_out, preferred_element_type=jnp.float32)
        embedded = updated.astype(jnp.bfloat16).reshape(BLK_DEV, ROWS, D)
        row_scores = lax.optimization_barrier(jnp.sum(layer_norm(updated, 1.0) * score_vec, axis=-1)).reshape(BLK_DEV, ROWS)
        live_mask = jnp.arange(ROWS, dtype=jnp.int32)[None, :] < lives[:, None]
        return (embedded, jnp.where(live_mask, row_scores, jnp.zeros_like(row_scores)))
    embedded_all, scores_all = lax.map(one_device, grouped)
    return (embedded_all.reshape(BLOCKS, ROWS, D), scores_all.reshape(BLOCKS, ROWS))
```

```python
import jax
import jax.numpy as jnp
from jax import lax
from jax.experimental import pallas as pl
from jax.experimental.pallas import tpu as pltpu
from jax.sharding import PartitionSpec as P


HEADS = 8
CORES = 2


epsilon = 1e-05


def layer_norm(values, gain):
    average = jnp.mean(values, axis=-1, keepdims=True)
    centred = values - average
    spread = jnp.mean(centred * centred, axis=-1, keepdims=True)
    return centred * lax.rsqrt(spread + epsilon) * gain


def shards(
    candidates,
    block_user,
    live_rows,
    prefix_keys,
    prefix_values,
    w_proj,
    w_out,
    gain_in,
    gain_mid,
    score_vec,
):
    helpers = lax.axis_size("helper")
    blocks, rows_block, features = candidates.shape
    head_dim = features // HEADS
    score_scale = head_dim ** (-0.5)
    proj_full, out_full = (
        lax.all_gather(w_proj, ("group", "helper"), axis=0, tiled=True),
        lax.all_gather(w_out, ("group", "helper"), axis=0, tiled=True),
    )
    cand_rows = candidates.reshape(blocks * rows_block, features).astype(jnp.float32)
    normed = layer_norm(cand_rows, gain_in).astype(jnp.bfloat16)
    projected = jax.nn.silu(jnp.dot(normed, proj_full, preferred_element_type=jnp.float32))
    gate_portion = projected[:, :features]
    value_part = projected[:, features : 2 * features]
    query_portion = projected[:, 2 * features : 3 * features]
    key_part = projected[:, 3 * features :]
    query_bf = lax.optimization_barrier(query_portion.astype(jnp.bfloat16))
    query_heads = query_bf.astype(jnp.float32).reshape(-1, HEADS, head_dim)
    own_weight = jax.nn.silu(
        score_scale * jnp.sum(query_heads * key_part.reshape(-1, HEADS, head_dim), axis=-1)
    )
    own_term = (own_weight[..., None] * value_part.reshape(-1, HEADS, head_dim)).reshape(
        -1, features
    )
    onehot = (block_user[None, :] == jnp.arange(helpers, dtype=jnp.int32)[:, None]).astype(
        jnp.bfloat16
    )
    outgoing = jnp.dot(
        onehot, query_bf.reshape(blocks, rows_block * features), preferred_element_type=jnp.float32
    )
    outgoing = outgoing.astype(jnp.bfloat16).reshape(helpers, rows_block, features)
    per_head_keys = prefix_keys[0].reshape(-1, HEADS, head_dim)
    per_head_values = prefix_values[0].reshape(-1, HEADS, head_dim)

    def attended_row_set(query_tile_group):
        raw_scores = jnp.einsum(
            "ocy,qcy->coq", query_tile_group, per_head_keys, preferred_element_type=jnp.float32
        )
        weight_brainfloat = jax.nn.silu(score_scale * raw_scores).astype(jnp.bfloat16)
        return jnp.einsum(
            "txw,wta->xta", weight_brainfloat, per_head_values, preferred_element_type=jnp.float32
        ).astype(jnp.bfloat16)

    arrived = lax.all_to_all(outgoing, "helper", split_axis=0, concat_axis=0, tiled=True)
    arrived_shape = arrived.shape
    count_rows = arrived_shape[0] * arrived_shape[1]
    flat_query = arrived.reshape(count_rows, HEADS, head_dim)
    if count_rows > 512 and count_rows % 512 == 0:
        mixed_heads = lax.map(
            attended_row_set, flat_query.reshape(count_rows // 512, 512, HEADS, head_dim)
        )
    else:
        mixed_heads = attended_row_set(flat_query)
    returned = lax.all_to_all(
        mixed_heads.reshape(arrived_shape), "helper", split_axis=0, concat_axis=0, tiled=True
    )
    prefix_mix = jnp.einsum(
        "jb,jf->bf",
        onehot,
        returned.reshape(helpers, rows_block * features),
        preferred_element_type=jnp.float32,
    )
    mixed = prefix_mix.reshape(-1, features) + own_term
    gated = (layer_norm(mixed, gain_mid) * gate_portion).astype(jnp.bfloat16)
    updated = cand_rows + jnp.dot(gated, out_full, preferred_element_type=jnp.float32)
    embeddings = updated.astype(jnp.bfloat16).reshape(blocks, rows_block, features)
    row_scores = jnp.sum(layer_norm(updated, 1.0) * score_vec, axis=-1).reshape(blocks, rows_block)
    live_mask = jnp.arange(rows_block, dtype=jnp.int32)[None, :] < live_rows[:, None]
    scores = jnp.where(live_mask, row_scores, jnp.zeros_like(row_scores))
    return (embeddings, scores)


def silu(values):
    half = 0.5 * values
    return half + half * jnp.tanh(half)


def kernel_call(body, out_shape, in_specs, scratch, out_specs=None, flops=0, vmem=16):
    any_or_vmem = out_specs
    if any_or_vmem is None:
        any_or_vmem = jax.tree.map(lambda _: pl.BlockSpec(memory_space=pltpu.VMEM), out_shape)
    return pl.pallas_call(
        body,
        out_shape=out_shape,
        in_specs=in_specs,
        out_specs=any_or_vmem,
        scratch_shapes=scratch,
        cost_estimate=pl.CostEstimate(flops=flops, transcendentals=0, bytes_accessed=1),
        compiler_params=pltpu.CompilerParams(vmem_limit_bytes=vmem * 1024 * 1024),
    )


ANY = pl.BlockSpec(memory_space=pltpu.HBM)


def in_hbm(arrays):
    return [pltpu.with_memory_space_constraint(array, pltpu.HBM) for array in arrays]


VMEM = pl.BlockSpec(memory_space=pltpu.VMEM)
SMEM = pl.BlockSpec(memory_space=pltpu.SMEM)


def columns_for_peers(array, parts, helpers):
    lead, width = array.shape[:-1], array.shape[-1]
    features = width // parts
    feats = features // helpers

    def body(in_ref, *outs):
        mine = lax.axis_index("helper")
        for rel in range(helpers):
            start = pl.multiple_of((mine ^ rel) * feats, feats)
            for part in range(parts):
                outs[rel][..., pl.ds(part * feats, feats)] = in_ref[
                    ..., pl.ds(part * features + start, feats)
                ]

    return kernel_call(body, [jax.ShapeDtypeStruct(lead + (parts * feats,), array.dtype)] * helpers, [VMEM], [])(array)


def weight_copies(refs, scratch, sems, rows, helpers, planes):
    group, mine = lax.axis_index("group"), lax.axis_index("helper")
    plane, core = group // CORES, lax.rem(group, CORES)
    copies = []
    for at, ref in enumerate(refs):
        turn, swap = at // CORES, at % CORES
        source = lax.rem(plane + planes - turn, planes) * CORES + (core ^ swap)
        for rel in range(helpers):
            start = pl.multiple_of((source * helpers + (mine ^ rel)) * rows, rows)
            copies.append(
                pltpu.make_async_copy(
                    ref.at[pl.ds(rel * rows, rows)], scratch.at[pl.ds(start, rows)], sems.at[len(copies)]
                )
            )
    return copies


def attend(cands, weights, prefixes, users, gain, rows, planes, rows_block):
    helpers = len(prefixes)
    (_, _, first), *_ = cands
    count, features = first.shape
    n_cands = len(cands)
    width = weights[0].shape[1]
    feats = width // 4
    prefix = prefixes[0].shape[1]
    head_dim = features // HEADS
    heads = feats // head_dim
    scale = head_dim ** (-0.5)
    blocks = count // rows_block
    n_weights = len(weights)

    def body(users_ref, gain_ref, *rest):
        cand_refs, rest = rest[:n_cands], rest[n_cands:]
        weight_refs, rest = rest[:n_weights], rest[n_weights:]
        prefix_refs, rest = rest[:helpers], rest[helpers:]
        mixed_ref, gate_ref, stats_ref = rest[:3]
        cand, normed, weight, keys, vals, proj, c_sems, w_sems, p_sems = rest[3:]
        c_copies = [
            pltpu.make_async_copy(ref, cand.at[rel, pl.ds(start, ref.shape[0])], c_sems.at[at])
            for at, ((rel, start, _), ref) in enumerate(zip(cands, cand_refs))
        ]
        p_copies = [
            pltpu.make_async_copy(
                prefix_refs[rel].at[part], held.at[pl.ds(rel * prefix, prefix)], p_sems.at[2 * rel + part]
            )
            for rel in range(helpers)
            for part, held in enumerate((keys, vals))
        ]
        w_copies = weight_copies(weight_refs, weight, w_sems, rows, helpers, planes)
        for copy in c_copies + w_copies + p_copies:
            copy.start()
        for rel in range(helpers):
            for (at, _, _), copy in zip(cands, c_copies):
                if at == rel:
                    copy.wait()
            values = cand[rel].astype(jnp.float32)
            average = jnp.mean(values, axis=-1, keepdims=True)
            centred = values - average
            spread = jnp.mean(centred * centred, axis=-1, keepdims=True)
            normed[rel] = (centred * lax.rsqrt(spread + epsilon) * gain_ref[...]).astype(jnp.bfloat16)
        for copy in w_copies:
            copy.wait()
        for copy in p_copies:
            copy.wait()
        lane = lax.broadcasted_iota(jnp.int32, (rows_block, 128), 1)
        for rel in range(helpers):
            proj[...] = silu(jnp.dot(normed[rel], weight[...], preferred_element_type=jnp.float32))
            gate_ref[pl.ds(rel * count, count)] = proj[:, :feats]
            for block in range(blocks):
                user = pl.multiple_of(users_ref[rel * blocks + block] * prefix, prefix)
                here = pl.ds(block * rows_block, rows_block)
                out = []
                for head in range(heads):
                    low = head * head_dim
                    val = proj[here, pl.ds(feats + low, head_dim)]
                    query = proj[here, pl.ds(2 * feats + low, head_dim)].astype(jnp.bfloat16)
                    key = proj[here, pl.ds(3 * feats + low, head_dim)]
                    own = silu(
                        scale * jnp.sum(query.astype(jnp.float32) * key, axis=-1, keepdims=True)
                    ) * val
                    raw = lax.dot_general(
                        query,
                        keys[pl.ds(user, prefix), pl.ds(low, head_dim)],
                        (((1,), (1,)), ((), ())),
                        preferred_element_type=jnp.float32,
                    )
                    share = silu(scale * raw).astype(jnp.bfloat16)
                    mix = jnp.dot(
                        share, vals[pl.ds(user, prefix), pl.ds(low, head_dim)], preferred_element_type=jnp.float32
                    )
                    out.append(mix.astype(jnp.bfloat16).astype(jnp.float32) + own)
                total = jnp.sum(sum(out), axis=-1, keepdims=True)
                average = total * (1.0 / feats)
                off = sum(jnp.sum((piece - average) ** 2, axis=-1, keepdims=True) for piece in out)
                both = jnp.where(lane == 0, average, jnp.where(lane == 1, off, 0.0))
                stats_ref[rel * blocks + block] = both.T[:8]
                for head in range(heads):
                    mixed_ref[
                        pl.ds(rel * count + block * rows_block, rows_block), pl.ds(head * head_dim, head_dim)
                    ] = out[head]

    total_rows = helpers * count
    shapes = [
        jax.ShapeDtypeStruct((total_rows, feats), jnp.float32),
        jax.ShapeDtypeStruct((total_rows, feats), jnp.float32),
        jax.ShapeDtypeStruct((helpers * blocks, 8, rows_block), jnp.float32),
    ]
    n_pieces = n_weights * helpers
    scratch = [
        pltpu.VMEM((helpers, count, features), jnp.bfloat16),
        pltpu.VMEM((helpers, count, features), jnp.bfloat16),
        pltpu.VMEM((features, width), jnp.bfloat16),
        pltpu.VMEM((helpers * prefix, feats), jnp.bfloat16),
        pltpu.VMEM((helpers * prefix, feats), jnp.bfloat16),
        pltpu.VMEM((count, width), jnp.float32),
        pltpu.SemaphoreType.DMA((n_cands,)),
        pltpu.SemaphoreType.DMA((n_pieces,)),
        pltpu.SemaphoreType.DMA((2 * helpers,)),
    ]
    arrays = in_hbm([array for _, _, array in cands] + list(weights) + list(prefixes))
    return kernel_call(
        body, shapes, [SMEM, VMEM] + [ANY] * len(arrays), scratch, flops=2 * total_rows * features * width
    )(users, gain, *arrays)


def gate(mixed, gates, stats, gain, helpers, rows_block):
    total_rows, feats = mixed.shape
    count = total_rows // helpers
    blocks = count // rows_block
    features = feats * helpers

    def body(mixed_ref, gate_ref, gain_ref, *rest):
        stats_refs, outs = rest[:helpers], rest[helpers:]
        for rel in range(helpers):
            for block in range(blocks):
                parts = [stats_refs[peer][(rel ^ peer) * blocks + block] for peer in range(helpers)]
                average = sum(part[0:1] for part in parts) * (1.0 / helpers)
                off = sum(
                    part[1:2] + feats * (part[0:1] - average) ** 2 for part in parts
                )
                level = lax.rsqrt(off * (1.0 / features) + epsilon)
                row = lax.broadcasted_iota(jnp.int32, (128, rows_block), 0)
                both = jnp.where(row == 0, average, jnp.where(row == 1, level, 0.0)).T
                here = pl.ds(rel * count + block * rows_block, rows_block)
                outs[rel][pl.ds(block * rows_block, rows_block)] = (
                    (mixed_ref[here] - both[:, 0:1]) * both[:, 1:2] * gain_ref[...] * gate_ref[here]
                ).astype(jnp.bfloat16)

    return kernel_call(
        body,
        [jax.ShapeDtypeStruct((count, feats), jnp.bfloat16)] * helpers,
        [VMEM] * (3 + helpers),
        [],
        flops=total_rows * feats * 8,
    )(mixed, gates, gain, *stats)


def project_out(gated, weights, cands, live, vec, rows, planes, rows_block):
    helpers = len(gated)
    count, features = cands.shape
    feats = features // helpers
    blocks = count // rows_block
    n_weights = len(weights)

    def body(live_ref, vec_ref, cand_ref, *rest):
        gated_refs = rest[:helpers]
        weight_refs = rest[helpers : helpers + n_weights]
        emb_ref, score_ref, weight, w_sems = rest[helpers + n_weights :]
        copies = weight_copies(weight_refs, weight, w_sems, rows, helpers, planes)
        for copy in copies:
            copy.start()
        for copy in copies:
            copy.wait()
        mine = lax.axis_index("helper")
        lane = lax.broadcasted_iota(jnp.int32, (1, rows_block), 1)
        for block in range(blocks):
            here = pl.ds(block * rows_block, rows_block)
            updated = cand_ref[here].astype(jnp.float32)
            moved = None
            for rel in range(helpers):
                start = pl.multiple_of((mine ^ rel) * feats, feats)
                part = jnp.dot(
                    gated_refs[rel][here], weight[pl.ds(start, feats)], preferred_element_type=jnp.float32
                )
                moved = part if moved is None else moved + part
            updated = updated + moved
            emb_ref[here] = updated.astype(jnp.bfloat16)
            average = jnp.mean(updated, axis=-1, keepdims=True)
            centred = updated - average
            spread = jnp.mean(centred * centred, axis=-1, keepdims=True)
            found = jnp.sum(centred * vec_ref[...], axis=-1, keepdims=True) * lax.rsqrt(spread + epsilon)
            across = jnp.broadcast_to(found, (rows_block, 128)).T[0:1]
            score_ref[pl.ds(block, 1)] = jnp.where(lane < live_ref[block], across, 0.0)

    shapes = [
        jax.ShapeDtypeStruct((count, features), jnp.bfloat16),
        jax.ShapeDtypeStruct((blocks, rows_block), jnp.float32),
    ]
    scratch = [
        pltpu.VMEM((features, features), jnp.bfloat16),
        pltpu.SemaphoreType.DMA((n_weights * helpers,)),
    ]
    return kernel_call(
        body,
        shapes,
        [SMEM] + [VMEM] * (2 + helpers) + [ANY] * n_weights,
        scratch,
        flops=2 * count * features * features,
    )(live, vec, cands, *gated, *in_hbm(weights))


def by_heads(
    candidates,
    block_user,
    live_rows,
    prefix_keys,
    prefix_values,
    w_proj,
    w_out,
    gain_in,
    gain_mid,
    score_vec,
):
    helpers, groups = lax.axis_size("helper"), lax.axis_size("group")
    planes = groups // CORES
    blocks, rows_block, features = candidates.shape
    feats = features // helpers
    rows = w_proj.shape[0]
    mine = lax.axis_index("helper")

    def sent(array, axis, pairs):
        return lax.ppermute(array, axis, pairs)

    def to_peers(pieces):
        return [pieces[0]] + [
            sent(pieces[rel], "helper", [(at, at ^ rel) for at in range(helpers)])
            for rel in range(1, len(pieces))
        ]

    def everyone(rows_here):
        if helpers != 4:
            return [(rel, 0, part) for rel, part in enumerate(to_peers([rows_here] * helpers))]
        near = to_peers([rows_here] * 3)
        half = rows_here.shape[0] // 2
        far = []
        for at, (over, of) in enumerate(((2, 1), (1, 2))):
            pairs = [(here, here ^ over) for here in range(helpers)]
            far.append((3, at * half, sent(near[of][at * half : (at + 1) * half], "helper", pairs)))
        return [(rel, 0, part) for rel, part in enumerate(near)] + far

    def spread(pieces):
        shard = jnp.concatenate(pieces, axis=0)
        out = []
        for turn in range(planes):
            held = shard
            if turn:
                pairs = [(at, (at + CORES * turn) % groups) for at in range(groups)]
                held = sent(shard, "group", pairs)
            swap = [(at, at ^ 1) for at in range(groups)]
            out += [held, sent(held, "group", swap)]
        return out

    cand_rows = candidates.reshape(blocks * rows_block, features)
    w_pieces = columns_for_peers(w_proj, 4, helpers)
    both = jnp.concatenate([prefix_keys, prefix_values], axis=0)
    prefix_pieces = columns_for_peers(both, 1, helpers)
    proj_shards = spread(to_peers(w_pieces))
    cands = everyone(cand_rows)
    prefixes = to_peers(prefix_pieces)
    users = jnp.concatenate(to_peers([block_user] * helpers)) ^ mine
    out_shards = spread(to_peers([w_out] * helpers))

    mixed, gates, stats = attend(
        cands, proj_shards, prefixes, users, gain_in.reshape(1, features), rows, planes, rows_block
    )
    all_stats = to_peers([stats] * helpers)
    my_gain = lax.dynamic_slice_in_dim(gain_mid.reshape(1, features), mine * feats, feats, axis=1)
    gated = gate(mixed, gates, all_stats, my_gain, helpers, rows_block)
    arrived = to_peers(gated)
    embeddings, scores = project_out(
        arrived, out_shards, cand_rows, live_rows, score_vec.reshape(1, features), rows, planes, rows_block
    )
    return embeddings.reshape(candidates.shape), scores


def whole(*arrays):
    return by_heads(*arrays)


def solution(mesh):
    helpers, groups = mesh.shape["helper"], mesh.shape["group"]
    split = HEADS % helpers == 0 and helpers & (helpers - 1) == 0 and groups % CORES == 0
    placed = (
        P(("group", "helper"), None, None),
        P(("group", "helper")),
        P(("group", "helper")),
        P(("group", "helper"), None, None),
        P(("group", "helper"), None, None),
        P(("group", "helper"), None),
        P(("group", "helper"), None),
        P(),
        P(),
        P(),
    )
    return jax.shard_map(
        whole if split else shards,
        mesh=mesh,
        in_specs=placed,
        out_specs=(P(("group", "helper"), None, None), P(("group", "helper"), None)),
        check_vma=False,
    )
```

```python
import jax
import jax.numpy as jnp
from jax import lax
from jax.experimental import pallas as pl
from jax.experimental.pallas import tpu as pltpu
from jax.sharding import PartitionSpec as P


HEADS = 8
CORES = 2
TAG_ROWS = 16


epsilon = 1e-05


def layer_norm(values, gain):
    average = jnp.mean(values, axis=-1, keepdims=True)
    centred = values - average
    spread = jnp.mean(centred * centred, axis=-1, keepdims=True)
    return centred * lax.rsqrt(spread + epsilon) * gain


def shards(
    candidates,
    block_user,
    live_rows,
    prefix_keys,
    prefix_values,
    w_proj,
    w_out,
    gain_in,
    gain_mid,
    score_vec,
):
    helpers = lax.axis_size("helper")
    blocks, rows_block, features = candidates.shape
    head_dim = features // HEADS
    score_scale = head_dim ** (-0.5)
    proj_full, out_full = (
        lax.all_gather(w_proj, ("group", "helper"), axis=0, tiled=True),
        lax.all_gather(w_out, ("group", "helper"), axis=0, tiled=True),
    )
    cand_rows = candidates.reshape(blocks * rows_block, features).astype(jnp.float32)
    normed = layer_norm(cand_rows, gain_in).astype(jnp.bfloat16)
    projected = jax.nn.silu(jnp.dot(normed, proj_full, preferred_element_type=jnp.float32))
    gate_portion = projected[:, :features]
    value_part = projected[:, features : 2 * features]
    query_portion = projected[:, 2 * features : 3 * features]
    key_part = projected[:, 3 * features :]
    query_bf = lax.optimization_barrier(query_portion.astype(jnp.bfloat16))
    query_heads = query_bf.astype(jnp.float32).reshape(-1, HEADS, head_dim)
    own_weight = jax.nn.silu(
        score_scale * jnp.sum(query_heads * key_part.reshape(-1, HEADS, head_dim), axis=-1)
    )
    own_term = (own_weight[..., None] * value_part.reshape(-1, HEADS, head_dim)).reshape(
        -1, features
    )
    onehot = (block_user[None, :] == jnp.arange(helpers, dtype=jnp.int32)[:, None]).astype(
        jnp.bfloat16
    )
    outgoing = jnp.dot(
        onehot, query_bf.reshape(blocks, rows_block * features), preferred_element_type=jnp.float32
    )
    outgoing = outgoing.astype(jnp.bfloat16).reshape(helpers, rows_block, features)
    per_head_keys = prefix_keys[0].reshape(-1, HEADS, head_dim)
    per_head_values = prefix_values[0].reshape(-1, HEADS, head_dim)

    def attended_row_set(query_tile_group):
        raw_scores = jnp.einsum(
            "ocy,qcy->coq", query_tile_group, per_head_keys, preferred_element_type=jnp.float32
        )
        weight_brainfloat = jax.nn.silu(score_scale * raw_scores).astype(jnp.bfloat16)
        return jnp.einsum(
            "txw,wta->xta", weight_brainfloat, per_head_values, preferred_element_type=jnp.float32
        ).astype(jnp.bfloat16)

    arrived = lax.all_to_all(outgoing, "helper", split_axis=0, concat_axis=0, tiled=True)
    arrived_shape = arrived.shape
    count_rows = arrived_shape[0] * arrived_shape[1]
    flat_query = arrived.reshape(count_rows, HEADS, head_dim)
    if count_rows > 512 and count_rows % 512 == 0:
        mixed_heads = lax.map(
            attended_row_set, flat_query.reshape(count_rows // 512, 512, HEADS, head_dim)
        )
    else:
        mixed_heads = attended_row_set(flat_query)
    returned = lax.all_to_all(
        mixed_heads.reshape(arrived_shape), "helper", split_axis=0, concat_axis=0, tiled=True
    )
    prefix_mix = jnp.einsum(
        "jb,jf->bf",
        onehot,
        returned.reshape(helpers, rows_block * features),
        preferred_element_type=jnp.float32,
    )
    mixed = prefix_mix.reshape(-1, features) + own_term
    gated = (layer_norm(mixed, gain_mid) * gate_portion).astype(jnp.bfloat16)
    updated = cand_rows + jnp.dot(gated, out_full, preferred_element_type=jnp.float32)
    embeddings = updated.astype(jnp.bfloat16).reshape(blocks, rows_block, features)
    row_scores = jnp.sum(layer_norm(updated, 1.0) * score_vec, axis=-1).reshape(blocks, rows_block)
    live_mask = jnp.arange(rows_block, dtype=jnp.int32)[None, :] < live_rows[:, None]
    scores = jnp.where(live_mask, row_scores, jnp.zeros_like(row_scores))
    return (embeddings, scores)


def silu(values):
    half = 0.5 * values
    return half + half * jnp.tanh(half)


def kernel_call(body, out_shape, in_specs, scratch, out_specs=None, flops=0, vmem=16):
    if out_specs is None:
        out_specs = jax.tree.map(lambda _: pl.BlockSpec(memory_space=pltpu.VMEM), out_shape)
    return pl.pallas_call(
        body,
        out_shape=out_shape,
        in_specs=in_specs,
        out_specs=out_specs,
        scratch_shapes=scratch,
        cost_estimate=pl.CostEstimate(flops=flops, transcendentals=0, bytes_accessed=1),
        compiler_params=pltpu.CompilerParams(vmem_limit_bytes=vmem * 1024 * 1024),
    )


ANY = pl.BlockSpec(memory_space=pltpu.HBM)


def in_hbm(arrays):
    return [pltpu.with_memory_space_constraint(array, pltpu.HBM) for array in arrays]


VMEM = pl.BlockSpec(memory_space=pltpu.VMEM)
SMEM = pl.BlockSpec(memory_space=pltpu.SMEM)


def columns_for_peers(arrays, parts, helpers):
    rows, width = arrays[0].shape[-2:]
    features = width // parts
    feats = features // helpers

    def body(*refs):
        in_refs, outs = refs[: len(arrays)], refs[len(arrays) :]
        mine = lax.axis_index("helper")
        for rel in range(helpers):
            start = pl.multiple_of((mine ^ rel) * feats, feats)
            for at, ref in enumerate(in_refs):
                for part in range(parts):
                    outs[rel][at, :, pl.ds(part * feats, feats)] = ref[:, pl.ds(part * features + start, feats)]

    return kernel_call(
        body,
        [jax.ShapeDtypeStruct((len(arrays), rows, parts * feats), arrays[0].dtype)] * helpers,
        [VMEM] * len(arrays),
        [],
    )(*arrays)


def prefix_for_peers(keys, values, users, helpers):
    prefix, features = keys.shape
    feats = features // helpers
    blocks = users.shape[0]

    def body(users_ref, k_ref, v_ref, *outs):
        mine = lax.axis_index("helper")
        row = lax.broadcasted_iota(jnp.int32, (TAG_ROWS, feats), 0)
        tags = jnp.zeros((TAG_ROWS, feats), jnp.int32)
        for block in range(blocks):
            tags = jnp.where(row == block, users_ref[block], tags)
        for rel in range(helpers):
            columns = pl.ds(pl.multiple_of((mine ^ rel) * feats, feats), feats)
            outs[rel][pl.ds(0, prefix)] = k_ref[:, columns]
            outs[rel][pl.ds(prefix, prefix)] = v_ref[:, columns]
            outs[rel][pl.ds(2 * prefix, TAG_ROWS)] = tags.astype(jnp.float32).astype(jnp.bfloat16)

    shape = (2 * prefix + TAG_ROWS, feats)
    return kernel_call(
        body,
        [pltpu.HBM(shape, keys.dtype)] + [jax.ShapeDtypeStruct(shape, keys.dtype)] * (helpers - 1),
        [SMEM, VMEM, VMEM],
        [],
        [VMEM] * helpers,
    )(*in_hbm([users, keys, values]))


def normalise(values, gain):
    average = jnp.mean(values, axis=-1, keepdims=True)
    centred = values - average
    spread = jnp.mean(centred * centred, axis=-1, keepdims=True)
    return (centred * lax.rsqrt(spread + epsilon) * gain).astype(jnp.bfloat16)


def norm_rows(arrays, gain, halves):
    def body(gain_ref, *refs):
        outs = list(refs[len(arrays) :])
        for ref in refs[: len(arrays)]:
            step = ref.shape[0] // halves
            for first in range(0, ref.shape[0], step):
                out = outs.pop(0)
                for at in range(0, step, 128):
                    out[pl.ds(at, 128)] = normalise(
                        ref[pl.ds(first + at, 128)].astype(jnp.float32), gain_ref[...]
                    )

    shapes = [
        pltpu.HBM((array.shape[0] // halves, array.shape[1]), jnp.bfloat16)
        for array in arrays
        for _ in range(halves)
    ]
    specs = [VMEM] * len(shapes)
    return kernel_call(body, shapes, [VMEM] * (1 + len(arrays)), [], specs)(*in_hbm([gain]), *arrays)


def weight_copies(refs, scratch, sems, rows, helpers, planes, by_plane):
    group, mine = lax.axis_index("group"), lax.axis_index("helper")
    plane, core = group // CORES, lax.rem(group, CORES)
    copies = []
    for at, ref in enumerate(refs):
        outer, swap = at // CORES, at % CORES
        for inner in range(helpers if by_plane else planes):
            turn, rel = (outer, inner) if by_plane else (inner, outer)
            source = ((plane ^ turn) * CORES + (core ^ swap)) * helpers + (mine ^ rel)
            copies.append(
                pltpu.make_async_copy(
                    ref.at[pl.ds(inner * rows, rows)],
                    scratch.at[pl.ds(pl.multiple_of(source * rows, rows), rows)],
                    sems.at[len(copies)],
                )
            )
    return copies


def attend(cands, weights, prefixes, rows, planes, rows_block):
    helpers = len(prefixes)
    count, features = sum(array.shape[0] for rel, _, array in cands if rel == 0), cands[0][2].shape[1]
    n_cands = len(cands)
    width = weights[0].shape[1]
    feats = width // 4
    prefix = (prefixes[0].shape[0] - TAG_ROWS) // 2
    head_dim = features // HEADS
    heads = feats // head_dim
    scale = head_dim ** (-0.5)
    blocks = count // rows_block
    n_weights = len(weights)

    def body(*rest):
        cand_refs, rest = rest[:n_cands], rest[n_cands:]
        weight_refs, rest = rest[:n_weights], rest[n_weights:]
        prefix_refs, rest = rest[:helpers], rest[helpers:]
        mixed_ref, gate_ref, stats_ref = rest[:3]
        normed, weight, keys, vals, tags, proj, c_sems, w_sems, p_sems, t_sems = rest[3:]
        c_copies = [
            pltpu.make_async_copy(ref, normed.at[rel, pl.ds(start, ref.shape[0])], c_sems.at[at])
            for at, ((rel, start, _), ref) in enumerate(zip(cands, cand_refs))
        ]
        p_copies = [
            pltpu.make_async_copy(
                prefix_refs[rel].at[pl.ds(part * prefix, prefix)],
                held.at[pl.ds(rel * prefix, prefix)],
                p_sems.at[2 * rel + part],
            )
            for rel in range(helpers)
            for part, held in enumerate((keys, vals))
        ]
        w_copies = weight_copies(weight_refs, weight, w_sems, rows, helpers, planes, True)
        t_copies = [
            pltpu.make_async_copy(
                prefix_refs[rel].at[pl.ds(2 * prefix, TAG_ROWS)], tags.at[rel], t_sems.at[rel]
            )
            for rel in range(helpers)
        ]
        for copy in t_copies + w_copies + c_copies + p_copies:
            copy.start()
        for copy in t_copies:
            copy.wait()
        mine = lax.axis_index("helper")
        owners = [
            jnp.max(tags[rel, pl.ds(block, 1), :128].astype(jnp.float32)).astype(jnp.int32) ^ mine
            for rel in range(helpers)
            for block in range(blocks)
        ]
        for copy in w_copies + c_copies:
            copy.wait()
        lane = lax.broadcasted_iota(jnp.int32, (rows_block, 128), 1)
        for rel in range(helpers):
            proj[...] = silu(jnp.dot(normed[rel], weight[...], preferred_element_type=jnp.float32))
            gate_ref[pl.ds(rel * count, count)] = proj[:, :feats]
            if rel == 0:
                for copy in p_copies:
                    copy.wait()
            for block in range(blocks):
                user = pl.multiple_of(owners[rel * blocks + block] * prefix, prefix)
                here = pl.ds(block * rows_block, rows_block)
                out = []
                for head in range(heads):
                    low = head * head_dim
                    val = proj[here, pl.ds(feats + low, head_dim)]
                    query = proj[here, pl.ds(2 * feats + low, head_dim)].astype(jnp.bfloat16)
                    key = proj[here, pl.ds(3 * feats + low, head_dim)]
                    own = silu(
                        scale * jnp.sum(query.astype(jnp.float32) * key, axis=-1, keepdims=True)
                    ) * val
                    raw = lax.dot_general(
                        query,
                        keys[pl.ds(user, prefix), pl.ds(low, head_dim)],
                        (((1,), (1,)), ((), ())),
                        preferred_element_type=jnp.float32,
                    )
                    share = silu(scale * raw).astype(jnp.bfloat16)
                    mix = jnp.dot(
                        share, vals[pl.ds(user, prefix), pl.ds(low, head_dim)], preferred_element_type=jnp.float32
                    )
                    out.append(mix.astype(jnp.bfloat16).astype(jnp.float32) + own)
                total = jnp.sum(sum(out), axis=-1, keepdims=True)
                average = total * (1.0 / feats)
                off = sum(jnp.sum((piece - average) ** 2, axis=-1, keepdims=True) for piece in out)
                both = jnp.where(lane == 0, average, jnp.where(lane == 1, off, 0.0))
                stats_ref[rel * blocks + block] = both.T[:8]
                for head in range(heads):
                    mixed_ref[
                        pl.ds(rel * count + block * rows_block, rows_block), pl.ds(head * head_dim, head_dim)
                    ] = out[head]

    total_rows = helpers * count
    shapes = [
        jax.ShapeDtypeStruct((total_rows, feats), jnp.float32),
        jax.ShapeDtypeStruct((total_rows, feats), jnp.float32),
        jax.ShapeDtypeStruct((helpers * blocks, 8, rows_block), jnp.float32),
    ]
    n_pieces = n_weights * helpers
    scratch = [
        pltpu.VMEM((helpers, count, features), jnp.bfloat16),
        pltpu.VMEM((features, width), jnp.bfloat16),
        pltpu.VMEM((helpers * prefix, feats), jnp.bfloat16),
        pltpu.VMEM((helpers * prefix, feats), jnp.bfloat16),
        pltpu.VMEM((helpers, TAG_ROWS, feats), jnp.bfloat16),
        pltpu.VMEM((count, width), jnp.float32),
        pltpu.SemaphoreType.DMA((n_cands,)),
        pltpu.SemaphoreType.DMA((n_pieces,)),
        pltpu.SemaphoreType.DMA((2 * helpers,)),
        pltpu.SemaphoreType.DMA((helpers,)),
    ]
    arrays = in_hbm([array for _, _, array in cands] + list(weights) + list(prefixes))
    return kernel_call(body, shapes, [ANY] * len(arrays), scratch, flops=2 * total_rows * features * width)(*arrays)


def gate(mixed, gates, stats, gain, helpers, rows_block):
    total_rows, feats = mixed.shape
    count = total_rows // helpers
    blocks = count // rows_block
    features = feats * helpers

    def body(mixed_ref, gate_ref, gain_ref, *rest):
        stats_refs, outs = rest[:helpers], rest[helpers:]
        mine = lax.axis_index("helper")
        my_gain = gain_ref[:, pl.ds(pl.multiple_of(mine * feats, feats), feats)]
        for rel in range(helpers):
            for block in range(blocks):
                parts = [stats_refs[peer][(rel ^ peer) * blocks + block] for peer in range(helpers)]
                average = sum(part[0:1] for part in parts) * (1.0 / helpers)
                off = sum(
                    part[1:2] + feats * (part[0:1] - average) ** 2 for part in parts
                )
                level = lax.rsqrt(off * (1.0 / features) + epsilon)
                row = lax.broadcasted_iota(jnp.int32, (128, rows_block), 0)
                both = jnp.where(row == 0, average, jnp.where(row == 1, level, 0.0)).T
                here = pl.ds(rel * count + block * rows_block, rows_block)
                outs[rel][pl.ds(block * rows_block, rows_block)] = (
                    (mixed_ref[here] - both[:, 0:1]) * both[:, 1:2] * my_gain * gate_ref[here]
                ).astype(jnp.bfloat16)

    return kernel_call(
        body,
        [jax.ShapeDtypeStruct((count, feats), jnp.bfloat16)] * helpers,
        [VMEM] * (3 + helpers),
        [],
        flops=total_rows * feats * 8,
    )(mixed, gates, gain, *stats)


def assemble(weights, rows, helpers, planes):
    n_weights = len(weights)
    width = weights[0].shape[1]
    features = CORES * planes * helpers * rows

    def body(*refs):
        weight_refs, out, sems = refs[:n_weights], refs[n_weights], refs[n_weights + 1]
        copies = weight_copies(weight_refs, out, sems, rows, helpers, planes, False)
        for copy in copies:
            copy.start()
        for copy in copies:
            copy.wait()

    return kernel_call(
        body,
        jax.ShapeDtypeStruct((features, width), weights[0].dtype),
        [ANY] * n_weights,
        [pltpu.SemaphoreType.DMA((n_weights * planes,))],
    )(*in_hbm(weights))


def project_out(gated, weight, cands, live, vec, rows_block):
    helpers = len(gated)
    count, features = cands.shape
    feats = features // helpers
    blocks = count // rows_block

    def body(live_ref, vec_ref, cand_ref, weight, *rest):
        gated_refs = rest[:helpers]
        emb_ref, score_ref = rest[helpers:]
        mine = lax.axis_index("helper")
        lane = lax.broadcasted_iota(jnp.int32, (1, rows_block), 1)
        for block in range(blocks):
            here = pl.ds(block * rows_block, rows_block)
            updated = cand_ref[here].astype(jnp.float32)
            moved = None
            for rel in range(helpers):
                start = pl.multiple_of((mine ^ rel) * feats, feats)
                part = jnp.dot(
                    gated_refs[rel][here], weight[pl.ds(start, feats)], preferred_element_type=jnp.float32
                )
                moved = part if moved is None else moved + part
            updated = updated + moved
            emb_ref[here] = updated.astype(jnp.bfloat16)
            average = jnp.mean(updated, axis=-1, keepdims=True)
            centred = updated - average
            spread = jnp.mean(centred * centred, axis=-1, keepdims=True)
            found = jnp.sum(centred * vec_ref[...], axis=-1, keepdims=True) * lax.rsqrt(spread + epsilon)
            across = jnp.broadcast_to(found, (rows_block, 128)).T[0:1]
            score_ref[pl.ds(block, 1)] = jnp.where(lane < live_ref[block], across, 0.0)

    shapes = [
        jax.ShapeDtypeStruct((count, features), jnp.bfloat16),
        jax.ShapeDtypeStruct((blocks, rows_block), jnp.float32),
    ]
    return kernel_call(
        body, shapes, [SMEM] + [VMEM] * (3 + helpers), [], flops=2 * count * features * features
    )(live, vec, cands, weight, *gated)


def by_heads(
    candidates,
    block_user,
    live_rows,
    prefix_keys,
    prefix_values,
    w_proj,
    w_out,
    gain_in,
    gain_mid,
    score_vec,
):
    helpers, groups = lax.axis_size("helper"), lax.axis_size("group")
    planes = groups // CORES
    blocks, rows_block, features = candidates.shape
    rows = w_proj.shape[0]

    def to_peers(pieces):
        return [pieces[0]] + [
            lax.ppermute(pieces[rel], "helper", [(at, at ^ rel) for at in range(helpers)])
            for rel in range(1, len(pieces))
        ]

    def everyone(rows_here, gain):
        near = to_peers([rows_here] * (3 if helpers == 4 else helpers))
        normed = norm_rows(near, gain, 2)
        half = rows_here.shape[0] // 2
        out = [(at // 2, at % 2 * half, part) for at, part in enumerate(normed)]
        if helpers == 4:
            for at, (over, part) in enumerate(((2, normed[2]), (1, normed[5]))):
                pairs = [(here, here ^ over) for here in range(helpers)]
                out.append((3, at * half, lax.ppermute(part, "helper", pairs)))
        return out

    def to_plane(array, turn):
        return lax.ppermute(array, "group", [(at, at ^ (CORES * turn)) for at in range(groups)])

    def to_core(array):
        return lax.ppermute(array, "group", [(here, here ^ 1) for here in range(groups)])

    def to_planes(shard):
        if planes != 4:
            return [shard] + [to_plane(shard, turn) for turn in range(1, planes)]
        near, across = to_plane(shard, 1), to_plane(shard, 2)
        inner = [CORES + core for core in range(CORES)]
        pairs = [(at, at ^ (3 * CORES)) for here in inner for at in (here, here + CORES)]
        middle = lax.ppermute(shard, "group", pairs)
        pairs = [(at, at ^ CORES) for here in inner for at in (here, here + CORES)]
        ends = lax.ppermute(across, "group", pairs)
        plane = lax.axis_index("group") // CORES
        return [shard, near, across, jnp.where((plane == 0) | (plane == 3), ends, middle)]

    def with_swaps(shards):
        return [part for shard in shards for part in (shard, to_core(shard))]

    cand_rows = candidates.reshape(blocks * rows_block, features)
    gain = gain_in.reshape(1, features)
    w_pieces = columns_for_peers(in_hbm([w_proj]), 4, helpers)
    prefix_pieces = prefix_for_peers(prefix_keys[0], prefix_values[0], block_user, helpers)
    w_shard = jnp.concatenate(to_peers([piece[0] for piece in w_pieces]), axis=0)
    proj_shards = with_swaps(to_planes(w_shard))
    cands = everyone(cand_rows, gain)
    prefixes = to_peers(prefix_pieces)
    o_shard = jnp.concatenate([w_out] + [to_plane(w_out, turn) for turn in range(1, planes)], axis=0)
    out_shards = with_swaps(to_peers([o_shard] * helpers))

    mixed, gates, stats = attend(
        cands, proj_shards, prefixes, rows, planes, rows_block
    )
    all_stats = to_peers([stats] * helpers)
    gated = gate(mixed, gates, all_stats, gain_mid.reshape(1, features), helpers, rows_block)
    arrived = to_peers(gated)
    out_full = assemble(out_shards, rows, helpers, planes)
    embeddings, scores = project_out(
        arrived, out_full, cand_rows, live_rows, score_vec.reshape(1, features), rows_block
    )
    return embeddings.reshape(candidates.shape), scores


def whole(*arrays):
    return by_heads(*arrays)


def solution(mesh):
    helpers, groups = mesh.shape["helper"], mesh.shape["group"]
    split = HEADS % helpers == 0 and helpers > 1 and groups % CORES == 0
    split = split and helpers & (helpers - 1) == 0 and groups & (groups - 1) == 0
    placed = (
        P(("group", "helper"), None, None),
        P(("group", "helper")),
        P(("group", "helper")),
        P(("group", "helper"), None, None),
        P(("group", "helper"), None, None),
        P(("group", "helper"), None),
        P(("group", "helper"), None),
        P(),
        P(),
        P(),
    )
    return jax.shard_map(
        whole if split else shards,
        mesh=mesh,
        in_specs=placed,
        out_specs=(P(("group", "helper"), None, None), P(("group", "helper"), None)),
        check_vma=False,
    )
```

```python
import jax
import jax.numpy as jnp
from jax import lax
from jax.experimental import pallas as pl
from jax.experimental.pallas import tpu as pltpu
from jax.sharding import PartitionSpec as P


HEADS = 8
CORES = 2
TAG_ROWS = 16


epsilon = 1e-05


def layer_norm(values, gain):
    average = jnp.mean(values, axis=-1, keepdims=True)
    centred = values - average
    spread = jnp.mean(centred * centred, axis=-1, keepdims=True)
    return centred * lax.rsqrt(spread + epsilon) * gain


def shards(
    candidates,
    block_user,
    live_rows,
    prefix_keys,
    prefix_values,
    w_proj,
    w_out,
    gain_in,
    gain_mid,
    score_vec,
):
    helpers = lax.axis_size("helper")
    blocks, rows_block, features = candidates.shape
    head_dim = features // HEADS
    score_scale = head_dim ** (-0.5)
    proj_full, out_full = (
        lax.all_gather(w_proj, ("group", "helper"), axis=0, tiled=True),
        lax.all_gather(w_out, ("group", "helper"), axis=0, tiled=True),
    )
    cand_rows = candidates.reshape(blocks * rows_block, features).astype(jnp.float32)
    normed = layer_norm(cand_rows, gain_in).astype(jnp.bfloat16)
    projected = jax.nn.silu(jnp.dot(normed, proj_full, preferred_element_type=jnp.float32))
    gate_portion = projected[:, :features]
    value_part = projected[:, features : 2 * features]
    query_portion = projected[:, 2 * features : 3 * features]
    key_part = projected[:, 3 * features :]
    query_bf = lax.optimization_barrier(query_portion.astype(jnp.bfloat16))
    query_heads = query_bf.astype(jnp.float32).reshape(-1, HEADS, head_dim)
    own_weight = jax.nn.silu(
        score_scale * jnp.sum(query_heads * key_part.reshape(-1, HEADS, head_dim), axis=-1)
    )
    own_term = (own_weight[..., None] * value_part.reshape(-1, HEADS, head_dim)).reshape(
        -1, features
    )
    onehot = (block_user[None, :] == jnp.arange(helpers, dtype=jnp.int32)[:, None]).astype(
        jnp.bfloat16
    )
    outgoing = jnp.dot(
        onehot, query_bf.reshape(blocks, rows_block * features), preferred_element_type=jnp.float32
    )
    outgoing = outgoing.astype(jnp.bfloat16).reshape(helpers, rows_block, features)
    per_head_keys = prefix_keys[0].reshape(-1, HEADS, head_dim)
    per_head_values = prefix_values[0].reshape(-1, HEADS, head_dim)

    def attended_row_set(query_tile_group):
        raw_scores = jnp.einsum(
            "ocy,qcy->coq", query_tile_group, per_head_keys, preferred_element_type=jnp.float32
        )
        weight_brainfloat = jax.nn.silu(score_scale * raw_scores).astype(jnp.bfloat16)
        return jnp.einsum(
            "txw,wta->xta", weight_brainfloat, per_head_values, preferred_element_type=jnp.float32
        ).astype(jnp.bfloat16)

    arrived = lax.all_to_all(outgoing, "helper", split_axis=0, concat_axis=0, tiled=True)
    arrived_shape = arrived.shape
    count_rows = arrived_shape[0] * arrived_shape[1]
    flat_query = arrived.reshape(count_rows, HEADS, head_dim)
    if count_rows > 512 and count_rows % 512 == 0:
        mixed_heads = lax.map(
            attended_row_set, flat_query.reshape(count_rows // 512, 512, HEADS, head_dim)
        )
    else:
        mixed_heads = attended_row_set(flat_query)
    returned = lax.all_to_all(
        mixed_heads.reshape(arrived_shape), "helper", split_axis=0, concat_axis=0, tiled=True
    )
    prefix_mix = jnp.einsum(
        "jb,jf->bf",
        onehot,
        returned.reshape(helpers, rows_block * features),
        preferred_element_type=jnp.float32,
    )
    mixed = prefix_mix.reshape(-1, features) + own_term
    gated = (layer_norm(mixed, gain_mid) * gate_portion).astype(jnp.bfloat16)
    updated = cand_rows + jnp.dot(gated, out_full, preferred_element_type=jnp.float32)
    embeddings = updated.astype(jnp.bfloat16).reshape(blocks, rows_block, features)
    row_scores = jnp.sum(layer_norm(updated, 1.0) * score_vec, axis=-1).reshape(blocks, rows_block)
    live_mask = jnp.arange(rows_block, dtype=jnp.int32)[None, :] < live_rows[:, None]
    scores = jnp.where(live_mask, row_scores, jnp.zeros_like(row_scores))
    return (embeddings, scores)


def silu(values):
    half = 0.5 * values
    return half + half * jnp.tanh(half)


def kernel_call(body, out_shape, in_specs, scratch, out_specs=None, flops=0, vmem=16):
    if out_specs is None:
        out_specs = jax.tree.map(lambda _: pl.BlockSpec(memory_space=pltpu.VMEM), out_shape)
    return pl.pallas_call(
        body,
        out_shape=out_shape,
        in_specs=in_specs,
        out_specs=out_specs,
        scratch_shapes=scratch,
        cost_estimate=pl.CostEstimate(flops=flops, transcendentals=0, bytes_accessed=1),
        compiler_params=pltpu.CompilerParams(vmem_limit_bytes=vmem * 1024 * 1024),
    )


ANY = pl.BlockSpec(memory_space=pltpu.HBM)


def in_hbm(arrays):
    return [pltpu.with_memory_space_constraint(array, pltpu.HBM) for array in arrays]


VMEM = pl.BlockSpec(memory_space=pltpu.VMEM)
SMEM = pl.BlockSpec(memory_space=pltpu.SMEM)


def columns_for_peers(arrays, parts, helpers):
    rows, width = arrays[0].shape[-2:]
    features = width // parts
    feats = features // helpers

    def body(*refs):
        in_refs, outs = refs[: len(arrays)], refs[len(arrays) :]
        mine = lax.axis_index("helper")
        for rel in range(helpers):
            start = pl.multiple_of((mine ^ rel) * feats, feats)
            for at, ref in enumerate(in_refs):
                for part in range(parts):
                    outs[rel][at, :, pl.ds(part * feats, feats)] = ref[:, pl.ds(part * features + start, feats)]

    return kernel_call(
        body,
        [jax.ShapeDtypeStruct((len(arrays), rows, parts * feats), arrays[0].dtype)] * helpers,
        [VMEM] * len(arrays),
        [],
    )(*arrays)


def prefix_for_peers(keys, values, users, helpers):
    prefix, features = keys.shape
    feats = features // helpers
    blocks = users.shape[0]

    def body(users_ref, k_ref, v_ref, *outs):
        mine = lax.axis_index("helper")
        row = lax.broadcasted_iota(jnp.int32, (TAG_ROWS, feats), 0)
        tags = jnp.zeros((TAG_ROWS, feats), jnp.int32)
        for block in range(blocks):
            tags = jnp.where(row == block, users_ref[block], tags)
        for rel in range(helpers):
            columns = pl.ds(pl.multiple_of((mine ^ rel) * feats, feats), feats)
            outs[rel][pl.ds(0, prefix)] = k_ref[:, columns]
            outs[rel][pl.ds(prefix, prefix)] = v_ref[:, columns]
            outs[rel][pl.ds(2 * prefix, TAG_ROWS)] = tags.astype(jnp.float32).astype(jnp.bfloat16)

    shape = (2 * prefix + TAG_ROWS, feats)
    return kernel_call(
        body,
        [pltpu.HBM(shape, keys.dtype)] + [jax.ShapeDtypeStruct(shape, keys.dtype)] * (helpers - 1),
        [SMEM, VMEM, VMEM],
        [],
        [VMEM] * helpers,
    )(*in_hbm([users, keys, values]))


def stack(pieces):
    rows, width = pieces[0].shape

    def body(*refs):
        for at, ref in enumerate(refs[:-1]):
            refs[-1][pl.ds(at * rows, rows)] = ref[...]

    shape = jax.ShapeDtypeStruct((len(pieces) * rows, width), pieces[0].dtype)
    return kernel_call(body, shape, [VMEM] * len(pieces), [])(*pieces)


def normalise(values, gain):
    average = jnp.mean(values, axis=-1, keepdims=True)
    centred = values - average
    spread = jnp.mean(centred * centred, axis=-1, keepdims=True)
    return (centred * lax.rsqrt(spread + epsilon) * gain).astype(jnp.bfloat16)


def norm_rows(arrays, gain, halves):
    def body(gain_ref, *refs):
        outs = list(refs[len(arrays) :])
        for ref in refs[: len(arrays)]:
            step = ref.shape[0] // halves
            for first in range(0, ref.shape[0], step):
                out = outs.pop(0)
                for at in range(0, step, 128):
                    out[pl.ds(at, 128)] = normalise(
                        ref[pl.ds(first + at, 128)].astype(jnp.float32), gain_ref[...]
                    )

    shapes = [
        pltpu.HBM((array.shape[0] // halves, array.shape[1]), jnp.bfloat16)
        for array in arrays
        for _ in range(halves)
    ]
    specs = [VMEM] * len(shapes)
    return kernel_call(body, shapes, [VMEM] * (1 + len(arrays)), [], specs)(*in_hbm([gain]), *arrays)


def weight_copies(refs, scratch, sems, rows, helpers, planes, by_plane):
    group, mine = lax.axis_index("group"), lax.axis_index("helper")
    plane, core = group // CORES, lax.rem(group, CORES)
    copies = []
    for at, ref in enumerate(refs):
        outer, swap = at // CORES, at % CORES
        for inner in range(helpers if by_plane else planes):
            turn, rel = (outer, inner) if by_plane else (inner, outer)
            source = ((plane ^ turn) * CORES + (core ^ swap)) * helpers + (mine ^ rel)
            copies.append(
                pltpu.make_async_copy(
                    ref.at[pl.ds(inner * rows, rows)],
                    scratch.at[pl.ds(pl.multiple_of(source * rows, rows), rows)],
                    sems.at[len(copies)],
                )
            )
    return copies


def attend(cands, weights, prefixes, rows, planes, rows_block):
    helpers = len(prefixes)
    count, features = sum(array.shape[0] for rel, _, array in cands if rel == 0), cands[0][2].shape[1]
    n_cands = len(cands)
    width = weights[0].shape[1]
    feats = width // 4
    prefix = (prefixes[0].shape[0] - TAG_ROWS) // 2
    head_dim = features // HEADS
    heads = feats // head_dim
    scale = head_dim ** (-0.5)
    blocks = count // rows_block
    n_weights = len(weights)

    def body(*rest):
        cand_refs, rest = rest[:n_cands], rest[n_cands:]
        weight_refs, rest = rest[:n_weights], rest[n_weights:]
        prefix_refs, rest = rest[:helpers], rest[helpers:]
        mixed_ref, gate_ref, stats_ref = rest[:3]
        normed, weight, keys, vals, tags, proj, c_sems, w_sems, p_sems, t_sems = rest[3:]
        c_copies = [
            pltpu.make_async_copy(ref, normed.at[rel, pl.ds(start, ref.shape[0])], c_sems.at[at])
            for at, ((rel, start, _), ref) in enumerate(zip(cands, cand_refs))
        ]
        p_copies = [
            pltpu.make_async_copy(
                prefix_refs[rel].at[pl.ds(part * prefix, prefix)],
                held.at[pl.ds(rel * prefix, prefix)],
                p_sems.at[2 * rel + part],
            )
            for rel in range(helpers)
            for part, held in enumerate((keys, vals))
        ]
        w_copies = weight_copies(weight_refs, weight, w_sems, rows, helpers, planes, True)
        t_copies = [
            pltpu.make_async_copy(
                prefix_refs[rel].at[pl.ds(2 * prefix, TAG_ROWS)], tags.at[rel], t_sems.at[rel]
            )
            for rel in range(helpers)
        ]
        for copy in t_copies + w_copies + c_copies + p_copies:
            copy.start()
        for copy in t_copies:
            copy.wait()
        mine = lax.axis_index("helper")
        owners = [
            jnp.max(tags[rel, pl.ds(block, 1), :128].astype(jnp.float32)).astype(jnp.int32) ^ mine
            for rel in range(helpers)
            for block in range(blocks)
        ]
        late = [at for at, (rel, _, _) in enumerate(cands) if rel]
        for copy in w_copies + [c_copies[at] for at in range(n_cands) if at not in late]:
            copy.wait()
        lane = lax.broadcasted_iota(jnp.int32, (rows_block, 128), 1)
        for rel in range(helpers):
            proj[...] = silu(jnp.dot(normed[rel], weight[...], preferred_element_type=jnp.float32))
            gate_ref[pl.ds(rel * count, count)] = proj[:, :feats]
            if rel == 0:
                for copy in p_copies + [c_copies[at] for at in late]:
                    copy.wait()
            for block in range(blocks):
                user = pl.multiple_of(owners[rel * blocks + block] * prefix, prefix)
                here = pl.ds(block * rows_block, rows_block)
                out = []
                for head in range(heads):
                    low = head * head_dim
                    val = proj[here, pl.ds(feats + low, head_dim)]
                    query = proj[here, pl.ds(2 * feats + low, head_dim)].astype(jnp.bfloat16)
                    key = proj[here, pl.ds(3 * feats + low, head_dim)]
                    own = silu(
                        scale * jnp.sum(query.astype(jnp.float32) * key, axis=-1, keepdims=True)
                    ) * val
                    raw = lax.dot_general(
                        query,
                        keys[pl.ds(user, prefix), pl.ds(low, head_dim)],
                        (((1,), (1,)), ((), ())),
                        preferred_element_type=jnp.float32,
                    )
                    share = silu(scale * raw).astype(jnp.bfloat16)
                    mix = jnp.dot(
                        share, vals[pl.ds(user, prefix), pl.ds(low, head_dim)], preferred_element_type=jnp.float32
                    )
                    out.append(mix.astype(jnp.bfloat16).astype(jnp.float32) + own)
                total = jnp.sum(sum(out), axis=-1, keepdims=True)
                average = total * (1.0 / feats)
                off = sum(jnp.sum((piece - average) ** 2, axis=-1, keepdims=True) for piece in out)
                both = jnp.where(lane == 0, average, jnp.where(lane == 1, off, 0.0))
                stats_ref[pl.ds(2 * (rel * blocks + block), 2)] = both.T[:2]
                for head in range(heads):
                    mixed_ref[
                        pl.ds(rel * count + block * rows_block, rows_block), pl.ds(head * head_dim, head_dim)
                    ] = out[head]

    total_rows = helpers * count
    shapes = [
        jax.ShapeDtypeStruct((total_rows, feats), jnp.float32),
        jax.ShapeDtypeStruct((total_rows, feats), jnp.float32),
        jax.ShapeDtypeStruct((2 * helpers * blocks, rows_block), jnp.float32),
    ]
    n_pieces = n_weights * helpers
    scratch = [
        pltpu.VMEM((helpers, count, features), jnp.bfloat16),
        pltpu.VMEM((features, width), jnp.bfloat16),
        pltpu.VMEM((helpers * prefix, feats), jnp.bfloat16),
        pltpu.VMEM((helpers * prefix, feats), jnp.bfloat16),
        pltpu.VMEM((helpers, TAG_ROWS, feats), jnp.bfloat16),
        pltpu.VMEM((count, width), jnp.float32),
        pltpu.SemaphoreType.DMA((n_cands,)),
        pltpu.SemaphoreType.DMA((n_pieces,)),
        pltpu.SemaphoreType.DMA((2 * helpers,)),
        pltpu.SemaphoreType.DMA((helpers,)),
    ]
    arrays = in_hbm([array for _, _, array in cands] + list(weights)[:-CORES])
    arrays += list(weights)[-CORES:] + in_hbm(prefixes)
    return kernel_call(body, shapes, [ANY] * len(arrays), scratch, flops=2 * total_rows * features * width)(*arrays)


def gate(mixed, gates, stats, gain, helpers, rows_block):
    total_rows, feats = mixed.shape
    count = total_rows // helpers
    blocks = count // rows_block
    features = feats * helpers

    def body(mixed_ref, gate_ref, gain_ref, *rest):
        stats_refs, outs = rest[:helpers], rest[helpers:]
        mine = lax.axis_index("helper")
        my_gain = gain_ref[:, pl.ds(pl.multiple_of(mine * feats, feats), feats)]
        for rel in range(helpers):
            for block in range(blocks):
                parts = [
                    stats_refs[peer][pl.ds(2 * ((rel ^ peer) * blocks + block), 2)] for peer in range(helpers)
                ]
                average = sum(part[0:1] for part in parts) * (1.0 / helpers)
                off = sum(
                    part[1:2] + feats * (part[0:1] - average) ** 2 for part in parts
                )
                level = lax.rsqrt(off * (1.0 / features) + epsilon)
                row = lax.broadcasted_iota(jnp.int32, (128, rows_block), 0)
                both = jnp.where(row == 0, average, jnp.where(row == 1, level, 0.0)).T
                here = pl.ds(rel * count + block * rows_block, rows_block)
                outs[rel][pl.ds(block * rows_block, rows_block)] = (
                    (mixed_ref[here] - both[:, 0:1]) * both[:, 1:2] * my_gain * gate_ref[here]
                ).astype(jnp.bfloat16)

    return kernel_call(
        body,
        [jax.ShapeDtypeStruct((count, feats), jnp.bfloat16)] * helpers,
        [VMEM] * (3 + helpers),
        [],
        flops=total_rows * feats * 8,
    )(mixed, gates, gain, *stats)


def assemble(weights, rows, helpers, planes):
    n_weights = len(weights)
    width = weights[0].shape[1]
    features = CORES * planes * helpers * rows

    def body(*refs):
        weight_refs, out, sems = refs[:n_weights], refs[n_weights], refs[n_weights + 1]
        copies = weight_copies(weight_refs, out, sems, rows, helpers, planes, False)
        for copy in copies:
            copy.start()
        for copy in copies:
            copy.wait()

    return kernel_call(
        body,
        jax.ShapeDtypeStruct((features, width), weights[0].dtype),
        [ANY] * n_weights,
        [pltpu.SemaphoreType.DMA((n_weights * planes,))],
    )(*in_hbm(weights))


def project_out(gated, weight, cands, live, vec, rows_block):
    helpers = len(gated)
    count, features = cands.shape
    feats = features // helpers
    blocks = count // rows_block

    def body(live_ref, vec_ref, cand_ref, weight, *rest):
        gated_refs = rest[:helpers]
        emb_ref, score_ref = rest[helpers:]
        mine = lax.axis_index("helper")
        lane = lax.broadcasted_iota(jnp.int32, (1, rows_block), 1)
        for block in range(blocks):
            here = pl.ds(block * rows_block, rows_block)
            updated = cand_ref[here].astype(jnp.float32)
            moved = None
            for rel in range(helpers):
                start = pl.multiple_of((mine ^ rel) * feats, feats)
                part = jnp.dot(
                    gated_refs[rel][here], weight[pl.ds(start, feats)], preferred_element_type=jnp.float32
                )
                moved = part if moved is None else moved + part
            updated = updated + moved
            emb_ref[here] = updated.astype(jnp.bfloat16)
            average = jnp.mean(updated, axis=-1, keepdims=True)
            centred = updated - average
            spread = jnp.mean(centred * centred, axis=-1, keepdims=True)
            found = jnp.sum(centred * vec_ref[...], axis=-1, keepdims=True) * lax.rsqrt(spread + epsilon)
            across = jnp.broadcast_to(found, (rows_block, 128)).T[0:1]
            score_ref[pl.ds(block, 1)] = jnp.where(lane < live_ref[block], across, 0.0)

    shapes = [
        jax.ShapeDtypeStruct((count, features), jnp.bfloat16),
        jax.ShapeDtypeStruct((blocks, rows_block), jnp.float32),
    ]
    return kernel_call(
        body, shapes, [SMEM] + [VMEM] * (3 + helpers), [], flops=2 * count * features * features
    )(live, vec, cands, weight, *gated)


def by_heads(
    candidates,
    block_user,
    live_rows,
    prefix_keys,
    prefix_values,
    w_proj,
    w_out,
    gain_in,
    gain_mid,
    score_vec,
):
    helpers, groups = lax.axis_size("helper"), lax.axis_size("group")
    planes = groups // CORES
    blocks, rows_block, features = candidates.shape
    rows = w_proj.shape[0]

    def to_peers(pieces):
        return [pieces[0]] + [
            lax.ppermute(pieces[rel], "helper", [(at, at ^ rel) for at in range(helpers)])
            for rel in range(1, len(pieces))
        ]

    def everyone(rows_here, gain):
        near = to_peers([rows_here] * (3 if helpers == 4 else helpers))
        normed = list(norm_rows(near[:1], gain, 2))
        normed += norm_rows(near[1:], gain, 2)
        half = rows_here.shape[0] // 2
        out = [(at // 2, at % 2 * half, part) for at, part in enumerate(normed)]
        if helpers == 4:
            for at, (over, part) in enumerate(((2, normed[2]), (1, normed[5]))):
                pairs = [(here, here ^ over) for here in range(helpers)]
                out.append((3, at * half, lax.ppermute(part, "helper", pairs)))
        return out

    def to_plane(array, turn):
        return lax.ppermute(array, "group", [(at, at ^ (CORES * turn)) for at in range(groups)])

    def to_core(array):
        return lax.ppermute(array, "group", [(here, here ^ 1) for here in range(groups)])

    def to_planes(shard):
        if planes != 4:
            return [shard] + [to_plane(shard, turn) for turn in range(1, planes)]
        near, across = to_plane(shard, 1), to_plane(shard, 2)
        inner = [CORES + core for core in range(CORES)]
        pairs = [(at, at ^ (3 * CORES)) for here in inner for at in (here, here + CORES)]
        middle = lax.ppermute(shard, "group", pairs)
        pairs = [(at, at ^ CORES) for here in inner for at in (here, here + CORES)]
        ends = lax.ppermute(across, "group", pairs)
        plane = lax.axis_index("group") // CORES
        return [shard, near, across, jnp.where((plane == 0) | (plane == 3), ends, middle)]

    def with_swaps(shards):
        return [part for shard in shards for part in (shard, to_core(shard))]

    cand_rows = candidates.reshape(blocks * rows_block, features)
    gain = gain_in.reshape(1, features)
    w_pieces = columns_for_peers(in_hbm([w_proj]), 4, helpers)
    prefix_pieces = prefix_for_peers(prefix_keys[0], prefix_values[0], block_user, helpers)
    w_shard = jnp.concatenate(to_peers([piece[0] for piece in w_pieces]), axis=0)
    proj_shards = with_swaps(to_planes(w_shard))
    cands = everyone(cand_rows, gain)
    prefixes = to_peers(prefix_pieces)
    o_parts = [w_out] + [to_plane(w_out, turn) for turn in range(1, planes)]
    o_shard = stack(o_parts)
    out_shards = with_swaps(to_peers([o_shard] * helpers))

    mixed, gates, stats = attend(
        cands, proj_shards, prefixes, rows, planes, rows_block
    )
    all_stats = to_peers([stats] * helpers)
    gated = gate(mixed, gates, all_stats, gain_mid.reshape(1, features), helpers, rows_block)
    arrived = to_peers(gated)
    out_full = assemble(out_shards, rows, helpers, planes)
    embeddings, scores = project_out(
        arrived, out_full, cand_rows, live_rows, score_vec.reshape(1, features), rows_block
    )
    return embeddings.reshape(candidates.shape), scores


def whole(*arrays):
    return by_heads(*arrays)


def solution(mesh):
    helpers, groups = mesh.shape["helper"], mesh.shape["group"]
    split = HEADS % helpers == 0 and helpers > 1 and groups % CORES == 0
    split = split and helpers & (helpers - 1) == 0 and groups & (groups - 1) == 0
    placed = (
        P(("group", "helper"), None, None),
        P(("group", "helper")),
        P(("group", "helper")),
        P(("group", "helper"), None, None),
        P(("group", "helper"), None, None),
        P(("group", "helper"), None),
        P(("group", "helper"), None),
        P(),
        P(),
        P(),
    )
    return jax.shard_map(
        whole if split else shards,
        mesh=mesh,
        in_specs=placed,
        out_specs=(P(("group", "helper"), None, None), P(("group", "helper"), None)),
        check_vma=False,
    )
```

```python
import jax
import jax.numpy as jnp
from jax import lax
from jax.experimental import pallas as pl
from jax.experimental.pallas import tpu as pltpu
from jax.sharding import PartitionSpec as P


HEADS = 8
CORES = 2
TAG_ROWS = 16


epsilon = 1e-05


def layer_norm(values, gain):
    average = jnp.mean(values, axis=-1, keepdims=True)
    centred = values - average
    spread = jnp.mean(centred * centred, axis=-1, keepdims=True)
    return centred * lax.rsqrt(spread + epsilon) * gain


def shards(
    candidates,
    block_user,
    live_rows,
    prefix_keys,
    prefix_values,
    w_proj,
    w_out,
    gain_in,
    gain_mid,
    score_vec,
):
    helpers = lax.axis_size("helper")
    blocks, rows_block, features = candidates.shape
    head_dim = features // HEADS
    score_scale = head_dim ** (-0.5)
    proj_full, out_full = (
        lax.all_gather(w_proj, ("group", "helper"), axis=0, tiled=True),
        lax.all_gather(w_out, ("group", "helper"), axis=0, tiled=True),
    )
    cand_rows = candidates.reshape(blocks * rows_block, features).astype(jnp.float32)
    normed = layer_norm(cand_rows, gain_in).astype(jnp.bfloat16)
    projected = jax.nn.silu(jnp.dot(normed, proj_full, preferred_element_type=jnp.float32))
    gate_portion = projected[:, :features]
    value_part = projected[:, features : 2 * features]
    query_portion = projected[:, 2 * features : 3 * features]
    key_part = projected[:, 3 * features :]
    query_bf = lax.optimization_barrier(query_portion.astype(jnp.bfloat16))
    query_heads = query_bf.astype(jnp.float32).reshape(-1, HEADS, head_dim)
    own_weight = jax.nn.silu(
        score_scale * jnp.sum(query_heads * key_part.reshape(-1, HEADS, head_dim), axis=-1)
    )
    own_term = (own_weight[..., None] * value_part.reshape(-1, HEADS, head_dim)).reshape(
        -1, features
    )
    onehot = (block_user[None, :] == jnp.arange(helpers, dtype=jnp.int32)[:, None]).astype(
        jnp.bfloat16
    )
    outgoing = jnp.dot(
        onehot, query_bf.reshape(blocks, rows_block * features), preferred_element_type=jnp.float32
    )
    outgoing = outgoing.astype(jnp.bfloat16).reshape(helpers, rows_block, features)
    per_head_keys = prefix_keys[0].reshape(-1, HEADS, head_dim)
    per_head_values = prefix_values[0].reshape(-1, HEADS, head_dim)

    def attended_row_set(query_tile_group):
        raw_scores = jnp.einsum(
            "ocy,qcy->coq", query_tile_group, per_head_keys, preferred_element_type=jnp.float32
        )
        weight_brainfloat = jax.nn.silu(score_scale * raw_scores).astype(jnp.bfloat16)
        return jnp.einsum(
            "txw,wta->xta", weight_brainfloat, per_head_values, preferred_element_type=jnp.float32
        ).astype(jnp.bfloat16)

    arrived = lax.all_to_all(outgoing, "helper", split_axis=0, concat_axis=0, tiled=True)
    arrived_shape = arrived.shape
    count_rows = arrived_shape[0] * arrived_shape[1]
    flat_query = arrived.reshape(count_rows, HEADS, head_dim)
    if count_rows > 512 and count_rows % 512 == 0:
        mixed_heads = lax.map(
            attended_row_set, flat_query.reshape(count_rows // 512, 512, HEADS, head_dim)
        )
    else:
        mixed_heads = attended_row_set(flat_query)
    returned = lax.all_to_all(
        mixed_heads.reshape(arrived_shape), "helper", split_axis=0, concat_axis=0, tiled=True
    )
    prefix_mix = jnp.einsum(
        "jb,jf->bf",
        onehot,
        returned.reshape(helpers, rows_block * features),
        preferred_element_type=jnp.float32,
    )
    mixed = prefix_mix.reshape(-1, features) + own_term
    gated = (layer_norm(mixed, gain_mid) * gate_portion).astype(jnp.bfloat16)
    updated = cand_rows + jnp.dot(gated, out_full, preferred_element_type=jnp.float32)
    embeddings = updated.astype(jnp.bfloat16).reshape(blocks, rows_block, features)
    row_scores = jnp.sum(layer_norm(updated, 1.0) * score_vec, axis=-1).reshape(blocks, rows_block)
    live_mask = jnp.arange(rows_block, dtype=jnp.int32)[None, :] < live_rows[:, None]
    scores = jnp.where(live_mask, row_scores, jnp.zeros_like(row_scores))
    return (embeddings, scores)


def silu(values):
    half = 0.5 * values
    return half + half * jnp.tanh(half)


def kernel_call(body, out_shape, in_specs, scratch, out_specs=None, flops=0, vmem=16):
    if out_specs is None:
        out_specs = jax.tree.map(lambda _: pl.BlockSpec(memory_space=pltpu.VMEM), out_shape)
    return pl.pallas_call(
        body,
        out_shape=out_shape,
        in_specs=in_specs,
        out_specs=out_specs,
        scratch_shapes=scratch,
        cost_estimate=pl.CostEstimate(flops=flops, transcendentals=0, bytes_accessed=1),
        compiler_params=pltpu.CompilerParams(vmem_limit_bytes=vmem * 1024 * 1024),
    )


ANY = pl.BlockSpec(memory_space=pltpu.HBM)


def in_hbm(arrays):
    return [pltpu.with_memory_space_constraint(array, pltpu.HBM) for array in arrays]


VMEM = pl.BlockSpec(memory_space=pltpu.VMEM)
SMEM = pl.BlockSpec(memory_space=pltpu.SMEM)


def columns_for_peers(arrays, parts, helpers):
    rows, width = arrays[0].shape[-2:]
    features = width // parts
    feats = features // helpers

    def body(*refs):
        in_refs, outs = refs[: len(arrays)], refs[len(arrays) :]
        mine = lax.axis_index("helper")
        for rel in range(helpers):
            start = pl.multiple_of((mine ^ rel) * feats, feats)
            for at, ref in enumerate(in_refs):
                for part in range(parts):
                    outs[rel][at, :, pl.ds(part * feats, feats)] = ref[:, pl.ds(part * features + start, feats)]

    return kernel_call(
        body,
        [jax.ShapeDtypeStruct((len(arrays), rows, parts * feats), arrays[0].dtype)] * helpers,
        [VMEM] * len(arrays),
        [],
    )(*arrays)


def prefix_for_peers(keys, values, users, helpers):
    prefix, features = keys.shape
    feats = features // helpers
    blocks = users.shape[0]

    def body(users_ref, k_ref, v_ref, *outs):
        mine = lax.axis_index("helper")
        row = lax.broadcasted_iota(jnp.int32, (TAG_ROWS, feats), 0)
        tags = jnp.zeros((TAG_ROWS, feats), jnp.int32)
        for block in range(blocks):
            tags = jnp.where(row == block, users_ref[block], tags)
        for rel in range(helpers):
            columns = pl.ds(pl.multiple_of((mine ^ rel) * feats, feats), feats)
            outs[rel][pl.ds(0, prefix)] = k_ref[:, columns]
            outs[rel][pl.ds(prefix, prefix)] = v_ref[:, columns]
            outs[rel][pl.ds(2 * prefix, TAG_ROWS)] = tags.astype(jnp.float32).astype(jnp.bfloat16)

    shape = (2 * prefix + TAG_ROWS, feats)
    return kernel_call(
        body,
        [pltpu.HBM(shape, keys.dtype)] + [jax.ShapeDtypeStruct(shape, keys.dtype)] * (helpers - 1),
        [SMEM, VMEM, VMEM],
        [],
        [VMEM] * helpers,
    )(*in_hbm([users, keys, values]))


def stack(pieces):
    rows, width = pieces[0].shape

    def body(*refs):
        for at, ref in enumerate(refs[:-1]):
            refs[-1][pl.ds(at * rows, rows)] = ref[...]

    shape = jax.ShapeDtypeStruct((len(pieces) * rows, width), pieces[0].dtype)
    return kernel_call(body, shape, [VMEM] * len(pieces), [])(*pieces)


def normalise(values, gain):
    average = jnp.mean(values, axis=-1, keepdims=True)
    centred = values - average
    spread = jnp.mean(centred * centred, axis=-1, keepdims=True)
    return (centred * lax.rsqrt(spread + epsilon) * gain).astype(jnp.bfloat16)


def norm_rows(arrays, gain, halves):
    def body(gain_ref, *refs):
        outs = list(refs[len(arrays) :])
        for ref in refs[: len(arrays)]:
            step = ref.shape[0] // halves
            for first in range(0, ref.shape[0], step):
                out = outs.pop(0)
                for at in range(0, step, 128):
                    out[pl.ds(at, 128)] = normalise(
                        ref[pl.ds(first + at, 128)].astype(jnp.float32), gain_ref[...]
                    )

    shapes = [
        pltpu.HBM((array.shape[0] // halves, array.shape[1]), jnp.bfloat16)
        for array in arrays
        for _ in range(halves)
    ]
    specs = [VMEM] * len(shapes)
    return kernel_call(body, shapes, [VMEM] * (1 + len(arrays)), [], specs)(*in_hbm([gain]), *arrays)


def weight_copies(refs, scratch, sems, rows, helpers, planes, by_plane):
    group, mine = lax.axis_index("group"), lax.axis_index("helper")
    plane, core = group // CORES, lax.rem(group, CORES)
    copies = []
    for at, ref in enumerate(refs):
        outer, swap = at // CORES, at % CORES
        for inner in range(helpers if by_plane else planes):
            turn, rel = (outer, inner) if by_plane else (inner, outer)
            source = ((plane ^ turn) * CORES + (core ^ swap)) * helpers + (mine ^ rel)
            copies.append(
                pltpu.make_async_copy(
                    ref.at[pl.ds(inner * rows, rows)],
                    scratch.at[pl.ds(pl.multiple_of(source * rows, rows), rows)],
                    sems.at[len(copies)],
                )
            )
    return copies


def attend(cands, weights, prefixes, rows, planes, rows_block):
    helpers = len(prefixes)
    count, features = sum(array.shape[0] for rel, _, array in cands if rel == 0), cands[0][2].shape[1]
    n_cands = len(cands)
    width = weights[0].shape[1]
    feats = width // 4
    prefix = (prefixes[0].shape[0] - TAG_ROWS) // 2
    head_dim = features // HEADS
    heads = feats // head_dim
    scale = head_dim ** (-0.5)
    blocks = count // rows_block
    n_weights = len(weights)

    def body(*rest):
        cand_refs, rest = rest[:n_cands], rest[n_cands:]
        weight_refs, rest = rest[:n_weights], rest[n_weights:]
        prefix_refs, rest = rest[:helpers], rest[helpers:]
        mixed_ref, gate_ref, stats_ref = rest[:3]
        normed, weight, keys, vals, tags, proj, c_sems, w_sems, p_sems, t_sems = rest[3:]
        c_copies = [
            pltpu.make_async_copy(ref, normed.at[rel, pl.ds(start, ref.shape[0])], c_sems.at[at])
            for at, ((rel, start, _), ref) in enumerate(zip(cands, cand_refs))
        ]
        p_copies = [
            pltpu.make_async_copy(
                prefix_refs[rel].at[pl.ds(part * prefix, prefix)],
                held.at[pl.ds(rel * prefix, prefix)],
                p_sems.at[2 * rel + part],
            )
            for rel in range(helpers)
            for part, held in enumerate((keys, vals))
        ]
        w_copies = weight_copies(weight_refs, weight, w_sems, rows, helpers, planes, True)
        t_copies = [
            pltpu.make_async_copy(
                prefix_refs[rel].at[pl.ds(2 * prefix, TAG_ROWS)], tags.at[rel], t_sems.at[rel]
            )
            for rel in range(helpers)
        ]
        for copy in t_copies + w_copies + c_copies + p_copies:
            copy.start()
        for copy in t_copies:
            copy.wait()
        mine = lax.axis_index("helper")
        owners = [
            jnp.max(tags[rel, pl.ds(block, 1), :128].astype(jnp.float32)).astype(jnp.int32) ^ mine
            for rel in range(helpers)
            for block in range(blocks)
        ]
        late = [at for at, (rel, _, _) in enumerate(cands) if rel]
        for copy in w_copies + [c_copies[at] for at in range(n_cands) if at not in late]:
            copy.wait()
        lane = lax.broadcasted_iota(jnp.int32, (rows_block, 128), 1)
        for rel in range(helpers):
            proj[...] = silu(jnp.dot(normed[rel], weight[...], preferred_element_type=jnp.float32))
            gate_ref[pl.ds(rel * count, count)] = proj[:, :feats]
            if rel == 0:
                for copy in p_copies + [c_copies[at] for at in late]:
                    copy.wait()
            for block in range(blocks):
                user = pl.multiple_of(owners[rel * blocks + block] * prefix, prefix)
                here = pl.ds(block * rows_block, rows_block)
                out = []
                for head in range(heads):
                    low = head * head_dim
                    val = proj[here, pl.ds(feats + low, head_dim)]
                    query = proj[here, pl.ds(2 * feats + low, head_dim)].astype(jnp.bfloat16)
                    key = proj[here, pl.ds(3 * feats + low, head_dim)]
                    own = silu(
                        scale * jnp.sum(query.astype(jnp.float32) * key, axis=-1, keepdims=True)
                    ) * val
                    raw = lax.dot_general(
                        query,
                        keys[pl.ds(user, prefix), pl.ds(low, head_dim)],
                        (((1,), (1,)), ((), ())),
                        preferred_element_type=jnp.float32,
                    )
                    share = silu(scale * raw).astype(jnp.bfloat16)
                    mix = jnp.dot(
                        share, vals[pl.ds(user, prefix), pl.ds(low, head_dim)], preferred_element_type=jnp.float32
                    )
                    out.append(mix.astype(jnp.bfloat16).astype(jnp.float32) + own)
                total = jnp.sum(sum(out), axis=-1, keepdims=True)
                average = total * (1.0 / feats)
                off = sum(jnp.sum((piece - average) ** 2, axis=-1, keepdims=True) for piece in out)
                both = jnp.where(lane == 0, average, jnp.where(lane == 1, off, 0.0))
                stats_ref[pl.ds(2 * (rel * blocks + block), 2)] = both.T[:2]
                for head in range(heads):
                    mixed_ref[
                        pl.ds(rel * count + block * rows_block, rows_block), pl.ds(head * head_dim, head_dim)
                    ] = out[head]

    total_rows = helpers * count
    shapes = [
        jax.ShapeDtypeStruct((total_rows, feats), jnp.float32),
        jax.ShapeDtypeStruct((total_rows, feats), jnp.float32),
        jax.ShapeDtypeStruct((2 * helpers * blocks, rows_block), jnp.float32),
    ]
    n_pieces = n_weights * helpers
    scratch = [
        pltpu.VMEM((helpers, count, features), jnp.bfloat16),
        pltpu.VMEM((features, width), jnp.bfloat16),
        pltpu.VMEM((helpers * prefix, feats), jnp.bfloat16),
        pltpu.VMEM((helpers * prefix, feats), jnp.bfloat16),
        pltpu.VMEM((helpers, TAG_ROWS, feats), jnp.bfloat16),
        pltpu.VMEM((count, width), jnp.float32),
        pltpu.SemaphoreType.DMA((n_cands,)),
        pltpu.SemaphoreType.DMA((n_pieces,)),
        pltpu.SemaphoreType.DMA((2 * helpers,)),
        pltpu.SemaphoreType.DMA((helpers,)),
    ]
    arrays = [array if rel == helpers - 1 else in_hbm([array])[0] for rel, _, array in cands]
    arrays += in_hbm(list(weights)[:-CORES])
    arrays += list(weights)[-CORES:] + in_hbm(prefixes)
    return kernel_call(body, shapes, [ANY] * len(arrays), scratch, flops=2 * total_rows * features * width)(*arrays)


def gate(mixed, gates, stats, gain, helpers, rows_block):
    total_rows, feats = mixed.shape
    count = total_rows // helpers
    blocks = count // rows_block
    features = feats * helpers

    def body(mixed_ref, gate_ref, gain_ref, *rest):
        stats_refs, outs = rest[:helpers], rest[helpers:]
        mine = lax.axis_index("helper")
        my_gain = gain_ref[:, pl.ds(pl.multiple_of(mine * feats, feats), feats)]
        for rel in range(helpers):
            for block in range(blocks):
                parts = [
                    stats_refs[peer][pl.ds(2 * ((rel ^ peer) * blocks + block), 2)] for peer in range(helpers)
                ]
                average = sum(part[0:1] for part in parts) * (1.0 / helpers)
                off = sum(
                    part[1:2] + feats * (part[0:1] - average) ** 2 for part in parts
                )
                level = lax.rsqrt(off * (1.0 / features) + epsilon)
                row = lax.broadcasted_iota(jnp.int32, (128, rows_block), 0)
                both = jnp.where(row == 0, average, jnp.where(row == 1, level, 0.0)).T
                here = pl.ds(rel * count + block * rows_block, rows_block)
                outs[rel][pl.ds(block * rows_block, rows_block)] = (
                    (mixed_ref[here] - both[:, 0:1]) * both[:, 1:2] * my_gain * gate_ref[here]
                ).astype(jnp.bfloat16)

    return kernel_call(
        body,
        [jax.ShapeDtypeStruct((count, feats), jnp.bfloat16)] * helpers,
        [VMEM] * (3 + helpers),
        [],
        flops=total_rows * feats * 8,
    )(mixed, gates, gain, *stats)


def assemble(weights, rows, helpers, planes):
    n_weights = len(weights)
    width = weights[0].shape[1]
    features = CORES * planes * helpers * rows

    def body(*refs):
        weight_refs, out, sems = refs[:n_weights], refs[n_weights], refs[n_weights + 1]
        copies = weight_copies(weight_refs, out, sems, rows, helpers, planes, False)
        for copy in copies:
            copy.start()
        for copy in copies:
            copy.wait()

    return kernel_call(
        body,
        jax.ShapeDtypeStruct((features, width), weights[0].dtype),
        [ANY] * n_weights,
        [pltpu.SemaphoreType.DMA((n_weights * planes,))],
    )(*weights)


def project_out(gated, weight, cands, live, vec, rows_block):
    helpers = len(gated)
    count, features = cands.shape
    feats = features // helpers
    blocks = count // rows_block

    def body(live_ref, vec_ref, cand_ref, weight, *rest):
        gated_refs = rest[:helpers]
        emb_ref, score_ref = rest[helpers:]
        mine = lax.axis_index("helper")
        lane = lax.broadcasted_iota(jnp.int32, (1, rows_block), 1)
        for block in range(blocks):
            here = pl.ds(block * rows_block, rows_block)
            updated = cand_ref[here].astype(jnp.float32)
            moved = None
            for rel in range(helpers):
                start = pl.multiple_of((mine ^ rel) * feats, feats)
                part = jnp.dot(
                    gated_refs[rel][here], weight[pl.ds(start, feats)], preferred_element_type=jnp.float32
                )
                moved = part if moved is None else moved + part
            updated = updated + moved
            emb_ref[here] = updated.astype(jnp.bfloat16)
            average = jnp.mean(updated, axis=-1, keepdims=True)
            centred = updated - average
            spread = jnp.mean(centred * centred, axis=-1, keepdims=True)
            found = jnp.sum(centred * vec_ref[...], axis=-1, keepdims=True) * lax.rsqrt(spread + epsilon)
            across = jnp.broadcast_to(found, (rows_block, 128)).T[0:1]
            score_ref[pl.ds(block, 1)] = jnp.where(lane < live_ref[block], across, 0.0)

    shapes = [
        jax.ShapeDtypeStruct((count, features), jnp.bfloat16),
        jax.ShapeDtypeStruct((blocks, rows_block), jnp.float32),
    ]
    return kernel_call(
        body, shapes, [SMEM] + [VMEM] * (3 + helpers), [], flops=2 * count * features * features
    )(live, vec, cands, weight, *gated)


def by_heads(
    candidates,
    block_user,
    live_rows,
    prefix_keys,
    prefix_values,
    w_proj,
    w_out,
    gain_in,
    gain_mid,
    score_vec,
):
    helpers, groups = lax.axis_size("helper"), lax.axis_size("group")
    planes = groups // CORES
    blocks, rows_block, features = candidates.shape
    rows = w_proj.shape[0]

    def to_peers(pieces):
        return [pieces[0]] + [
            lax.ppermute(pieces[rel], "helper", [(at, at ^ rel) for at in range(helpers)])
            for rel in range(1, len(pieces))
        ]

    def everyone(rows_here, gain):
        near = to_peers([rows_here] * (3 if helpers == 4 else helpers))
        normed = list(norm_rows(near[:1], gain, 2))
        normed += norm_rows(near[1:], gain, 2)
        half = rows_here.shape[0] // 2
        out = [(at // 2, at % 2 * half, part) for at, part in enumerate(normed)]
        if helpers == 4:
            for at, (over, part) in enumerate(((2, normed[2]), (1, normed[5]))):
                pairs = [(here, here ^ over) for here in range(helpers)]
                out.append((3, at * half, lax.ppermute(part, "helper", pairs)))
        return out

    def to_plane(array, turn):
        return lax.ppermute(array, "group", [(at, at ^ (CORES * turn)) for at in range(groups)])

    def to_core(array):
        return lax.ppermute(array, "group", [(here, here ^ 1) for here in range(groups)])

    def to_planes(shard):
        if planes != 4:
            return [shard] + [to_plane(shard, turn) for turn in range(1, planes)]
        near, across = to_plane(shard, 1), to_plane(shard, 2)
        inner = [CORES + core for core in range(CORES)]
        pairs = [(at, at ^ (3 * CORES)) for here in inner for at in (here, here + CORES)]
        middle = lax.ppermute(shard, "group", pairs)
        pairs = [(at, at ^ CORES) for here in inner for at in (here, here + CORES)]
        ends = lax.ppermute(across, "group", pairs)
        plane = lax.axis_index("group") // CORES
        return [shard, near, across, jnp.where((plane == 0) | (plane == 3), ends, middle)]

    def with_swaps(shards):
        return [part for shard in shards for part in (shard, to_core(shard))]

    cand_rows = candidates.reshape(blocks * rows_block, features)
    gain = gain_in.reshape(1, features)
    w_pieces = columns_for_peers(in_hbm([w_proj]), 4, helpers)
    prefix_pieces = prefix_for_peers(prefix_keys[0], prefix_values[0], block_user, helpers)
    w_shard = jnp.concatenate(to_peers([piece[0] for piece in w_pieces]), axis=0)
    proj_shards = with_swaps(to_planes(w_shard))
    cands = everyone(cand_rows, gain)
    prefixes = to_peers(prefix_pieces)
    o_parts = [w_out] + [to_plane(w_out, turn) for turn in range(1, planes)]
    o_shard = stack(o_parts)
    out_shards = with_swaps(to_peers([o_shard] * helpers))

    mixed, gates, stats = attend(
        cands, proj_shards, prefixes, rows, planes, rows_block
    )
    all_stats = to_peers([stats] * helpers)
    gated = gate(mixed, gates, all_stats, gain_mid.reshape(1, features), helpers, rows_block)
    arrived = to_peers(gated)
    out_full = assemble(out_shards, rows, helpers, planes)
    embeddings, scores = project_out(
        arrived, out_full, cand_rows, live_rows, score_vec.reshape(1, features), rows_block
    )
    return embeddings.reshape(candidates.shape), scores


def whole(*arrays):
    return by_heads(*arrays)


def solution(mesh):
    helpers, groups = mesh.shape["helper"], mesh.shape["group"]
    split = HEADS % helpers == 0 and helpers > 1 and groups % CORES == 0
    split = split and helpers & (helpers - 1) == 0 and groups & (groups - 1) == 0
    placed = (
        P(("group", "helper"), None, None),
        P(("group", "helper")),
        P(("group", "helper")),
        P(("group", "helper"), None, None),
        P(("group", "helper"), None, None),
        P(("group", "helper"), None),
        P(("group", "helper"), None),
        P(),
        P(),
        P(),
    )
    return jax.shard_map(
        whole if split else shards,
        mesh=mesh,
        in_specs=placed,
        out_specs=(P(("group", "helper"), None, None), P(("group", "helper"), None)),
        check_vma=False,
    )
```
